32 devices in a mesh: dp: 8 (over y, x, core), tensor: 4 (over z).
Axes of the slice: x: 2, y: 2, z: 4, core: 2. Of those that a mesh axis runs over, the one named last changes fastest.
Arguments:
- text: bfloat16 [8, 256, 5120], P('dp', None, 'tensor'), may hold values from -6 to 6
- prompts: bfloat16 [8, 100, 5120], P('dp', None, 'tensor'), may hold values from -6 to 6
- gain: float32 [5120], replicated, may hold values from 0.1 to 1.9
- w_query: bfloat16 [5120, 3072], P(None, 'tensor'), may hold values from -0.069877124 to 0.069877124, as said below
- w_key: bfloat16 [5120, 3072], P(None, 'tensor'), may hold values from -1.2577882 to 1.2577882, as said below
- w_value: bfloat16 [5120, 3072], P(None, 'tensor'), may hold values from -0.078125 to 0.078125
- cotangent: bfloat16 [8, 356, 3072], P('dp', None, 'tensor'), may hold values from -6 to 6
- task_of: int32 [8], replicated, may hold values from 0 to 7, as said below
- lengths: int32 [8], replicated, may hold values from 1 to 256, as said below
- slot: int32 [8], replicated, may hold values from 0 to 7, as said below
Outputs:
- attn_out: bfloat16 [8, 356, 3072], P('dp', None, 'tensor')
- prompt_grad: float32 [8, 100, 5120], P('dp', None, 'tensor')
The draws below stay inside these ranges and needn't reach their ends.
Inputs may be any that keep to these rules, and one draw needn't show every extreme that they name: `task_of`: nondecreasing along the source order. `lengths`: some example has exactly 256 text tokens; rows of an example beyond its length are padding. `slot`: a permutation of 0 to 7; position s lies on index s // 1 of dp. `w_query`: entries of order 5120 ** -0.5. `w_key`: entries of order 5120 ** -0.5 or larger.
All inputs are finite; a program needn't handle non-finite values.
Results may differ from the reference program's by a relative error of at most 0.0082.
Values may be sent and summed in bfloat16 or wider, within the bound.
A program may use at most 128 MiB of HBM per device.

```python
import math
import jax
import jax.numpy as jnp
from jax import lax

D = 5120
HEADS = 24
HD = 128
P_SIZE = 100
SEQ = 256
EX_DEV = 1
ROWS = 356
EXAMPLES = 8
TASKS = 8


def weight_base(key):
    return jax.random.truncated_normal(jax.random.fold_in(key, 11), -4.0, 4.0, (D, HEADS * HD), jnp.float32) / math.sqrt(D)


def draw_w_query(key, part):
    return weight_base(key).astype(jnp.bfloat16)


def draw_w_key(key, part):
    noise_part = jax.random.truncated_normal(jax.random.fold_in(key, 12), -4.0, 4.0, (D, HEADS * HD), jnp.float32) / math.sqrt(D)
    result = noise_part
    return result.astype(jnp.bfloat16)


def draw_task_of(key, part):
    first_key, second_key, third_key = jax.random.split(jax.random.fold_in(key, 21), 3)
    first_pick = jax.random.randint(first_key, (EXAMPLES,), 0, TASKS)
    second_pick = jax.random.randint(second_key, (EXAMPLES,), 0, TASKS)
    ranked = jnp.minimum(first_pick, second_pick)
    shuffle = jax.random.permutation(third_key, TASKS)
    return jnp.sort(shuffle[ranked]).astype(jnp.int32)


def length_base(key):
    first_key, second_key = jax.random.split(jax.random.fold_in(key, 31))
    raw_lengths = jax.random.randint(first_key, (EXAMPLES,), 1, SEQ + 1)
    longest = jax.random.randint(second_key, (), 0, EXAMPLES)
    return jnp.where(jnp.arange(EXAMPLES) == longest, SEQ, raw_lengths).astype(jnp.int32)


def draw_lengths(key, part):
    return length_base(key)


def draw_slot(key, part):
    length_all = length_base(key)
    device_count = EXAMPLES // EX_DEV
    order = jnp.argsort(-length_all, stable=True)
    ranks = jnp.arange(EXAMPLES, dtype=jnp.int32)
    rounds = ranks // device_count
    column = ranks % device_count
    device = jnp.where(rounds % 2 == 0, column, device_count - 1 - column)
    placed = (device * EX_DEV + rounds).astype(jnp.int32)
    return jnp.zeros((EXAMPLES,), jnp.int32).at[order].set(placed)


def block_scale(key, dims, shards, least, largest):
    level, own = 1.0, jax.random.fold_in(key, 6)
    for dim, shards_of in shards:
        draws = jnp.exp(jax.random.uniform(jax.random.fold_in(own, dim), (shards_of,), jnp.float32, least / len(shards), largest / len(shards)))
        level = level * jnp.repeat(draws, dims[dim] // shards_of).reshape([-1 if axis == dim else 1 for axis in range(len(dims))])
    return level


def scatter_about(stream_key, shape, width, most, cuts=(), held_as=jnp.bfloat16):
    factor_of = block_scale(stream_key, shape, cuts, -0.22, 0.18) if cuts else 1.0
    array = jax.random.normal(stream_key, shape, jnp.float32) * width * factor_of
    return jnp.minimum(jnp.maximum(array, -most), most).astype(held_as)


def setup_inputs(seed: int = 0) -> dict:
    keys = jax.random.split(jax.random.key(seed), 11)
    return {
        "text": scatter_about(keys[0], (EXAMPLES, SEQ, D), 1.0, 6.0, ((0, 8), (2, 4))),
        "prompts": scatter_about(keys[1], (TASKS, P_SIZE, D), 1.0, 6.0, ((0, 8), (2, 4))),
        "gain": jnp.clip(1.0 + 0.18 * jax.random.normal(keys[2], (D,), jnp.float32), 0.1, 1.9),
        "w_query": draw_w_query(jax.random.fold_in(keys[10], 71), 0),
        "w_key": draw_w_key(jax.random.fold_in(keys[10], 71), 0),
        "w_value": scatter_about(keys[5], (D, HEADS * HD), D ** -0.5, 0.078125, ((1, 4),)),
        "cotangent": scatter_about(keys[6], (EXAMPLES, ROWS, HEADS * HD), 1.0, 6.0, ((0, 8), (2, 4))),
        "task_of": draw_task_of(jax.random.fold_in(keys[10], 71), 0),
        "lengths": draw_lengths(jax.random.fold_in(keys[10], 71), 0),
        "slot": draw_slot(jax.random.fold_in(keys[10], 71), 0),
    }


def rope_tables(row_count):
    half_dim = HD // 2
    frequency = 10000.0 ** (-jnp.arange(half_dim, dtype=jnp.float32) / half_dim)
    angle_table = jnp.arange(row_count, dtype=jnp.float32)[:, None] * frequency[None, :]
    return (jnp.cos(angle_table), jnp.sin(angle_table))

def rotate(vectors, cosine_table, sine_table):
    half_dim = vectors.shape[-1] // 2
    first_half = vectors[..., :half_dim]
    second_half = vectors[..., half_dim:]
    cosine_b = cosine_table[:, None, :]
    sine_b = sine_table[:, None, :]
    return jnp.concatenate([first_half * cosine_b - second_half * sine_b, second_half * cosine_b + first_half * sine_b], axis=-1)

def unrotate(vectors, cosine_table, sine_table):
    half_dim = vectors.shape[-1] // 2
    first_half = vectors[..., :half_dim]
    second_half = vectors[..., half_dim:]
    cosine_b = cosine_table[:, None, :]
    sine_b = sine_table[:, None, :]
    return jnp.concatenate([first_half * cosine_b + second_half * sine_b, second_half * cosine_b - first_half * sine_b], axis=-1)

def transpose_product(grad_low, matrix):
    return lax.dot_general(grad_low, matrix, (((1,), (1,)), ((), ())), preferred_element_type=jnp.float32)

def attention_window(full_rows, gain, w_query, w_key, w_value, cotangent, valid_rows, prompt_len):
    batch_size, row_count, model_width = full_rows.shape
    head_count = w_query.shape[1] // HD
    wide_rows = full_rows.astype(jnp.float32)
    inv_rms = lax.rsqrt(lax.optimization_barrier(jnp.mean(wide_rows * wide_rows, axis=-1)) + 1e-05)
    normed = (wide_rows * inv_rms[..., None] * gain).astype(jnp.bfloat16).reshape(batch_size * row_count, model_width)
    cosine_table, sine_table = rope_tables(row_count)

    def project(matrix):
        return jnp.dot(normed, matrix, preferred_element_type=jnp.float32).reshape(batch_size, row_count, head_count, HD)
    queries = rotate(project(w_query), cosine_table, sine_table).astype(jnp.bfloat16)
    key_rows = rotate(project(w_key), cosine_table, sine_table).astype(jnp.bfloat16)
    value_rows = project(w_value).astype(jnp.bfloat16)
    score_scale = 1.0 / math.sqrt(HD)
    scores = jnp.einsum('erhd,ekhd->ehrk', queries.astype(jnp.float32), key_rows.astype(jnp.float32)) * score_scale
    rows_at = jnp.arange(row_count, dtype=jnp.int32)
    row_limit = (prompt_len + valid_rows).astype(jnp.int32)
    allowed = (rows_at[None, None, :] <= rows_at[None, :, None]) & (rows_at[None, None, :] < row_limit[:, None, None])
    allowed = allowed[:, None]
    scores = jnp.where(allowed, scores, -1e+30)
    row_peak = lax.optimization_barrier(jnp.max(scores, axis=-1, keepdims=True))
    weights = jnp.where(allowed, jnp.exp(scores - row_peak), 0.0)
    probability = weights / lax.optimization_barrier(jnp.sum(weights, axis=-1, keepdims=True))
    probs_low = probability.astype(jnp.bfloat16)
    live_rows = rows_at[None, :] < row_limit[:, None]
    mixed_rows = jnp.einsum('ehrk,ekhd->erhd', probs_low.astype(jnp.float32), value_rows.astype(jnp.float32))
    mixed_rows = jnp.where(live_rows[:, :, None, None], mixed_rows, 0.0)
    output = mixed_rows.reshape(batch_size, row_count, head_count * HD).astype(jnp.bfloat16)
    upstream = jnp.where(live_rows[:, :, None, None], cotangent.reshape(batch_size, row_count, head_count, HD), 0.0).astype(jnp.bfloat16)
    grad_prob = jnp.einsum('erhd,ekhd->ehrk', upstream.astype(jnp.float32), value_rows.astype(jnp.float32))
    row_delta = lax.optimization_barrier(jnp.sum(probability * grad_prob, axis=-1, keepdims=True))
    grad_score = (probability * (grad_prob - row_delta)).astype(jnp.bfloat16)
    grad_query = jnp.einsum('ehrk,ekhd->erhd', grad_score[:, :, :prompt_len, :].astype(jnp.float32), key_rows.astype(jnp.float32)) * score_scale
    grad_key = jnp.einsum('ehrk,erhd->ekhd', grad_score[:, :, :, :prompt_len].astype(jnp.float32), queries.astype(jnp.float32)) * score_scale
    grad_value = jnp.einsum('ehrk,erhd->ekhd', probs_low[:, :, :, :prompt_len].astype(jnp.float32), upstream.astype(jnp.float32))
    cosine_lead = cosine_table[:prompt_len]
    sine_lead = sine_table[:prompt_len]
    flat_rows = batch_size * prompt_len
    grad_query = unrotate(grad_query, cosine_lead, sine_lead).astype(jnp.bfloat16).reshape(flat_rows, head_count * HD)
    grad_key = unrotate(grad_key, cosine_lead, sine_lead).astype(jnp.bfloat16).reshape(flat_rows, head_count * HD)
    grad_value = grad_value.astype(jnp.bfloat16).reshape(flat_rows, head_count * HD)
    grad_normed = transpose_product(grad_query, w_query) + transpose_product(grad_key, w_key) + transpose_product(grad_value, w_value)
    grad_normed = grad_normed.reshape(batch_size, prompt_len, model_width) * gain
    prompt_rows = wide_rows[:, :prompt_len]
    prompt_inv = inv_rms[:, :prompt_len, None]
    grad_rows = prompt_inv * grad_normed - prompt_rows * prompt_inv ** 3 * lax.optimization_barrier(jnp.mean(grad_normed * prompt_rows, axis=-1, keepdims=True))
    return (output, grad_rows)

def reference(text, prompts, gain, w_query, w_key, w_value, cotangent, task_of, lengths, slot):
    example_count = text.shape[0]
    positions = jnp.arange(example_count, dtype=jnp.int32)

    def one_slot(task_grads, place_id):
        hit_mask = slot == place_id
        source = jnp.sum(jnp.where(hit_mask, positions, 0)).astype(jnp.int32)
        task_id = jnp.sum(jnp.where(hit_mask, task_of, 0)).astype(jnp.int32)
        length = jnp.sum(jnp.where(hit_mask, lengths, 0)).astype(jnp.int32)
        joined = jnp.concatenate([prompts[task_id], text[source]], axis=0)[None]
        output, grad_rows = attention_window(joined, gain, w_query, w_key, w_value, cotangent[place_id][None], length[None], P_SIZE)
        task_grads = task_grads.at[task_id].add(grad_rows[0])
        return (task_grads, output[0])
    prompt_grad, attn_out = lax.scan(one_slot, jnp.zeros((TASKS, P_SIZE, D), jnp.float32), positions)
    return (attn_out, prompt_grad)
```

```python
import functools
import math

import jax
import jax.numpy as jnp
import numpy as np
from jax import lax
from jax.experimental import pallas as pl
from jax.experimental.pallas import tpu as pltpu
from jax.sharding import PartitionSpec as P

HD = 128


def rope_tables(row_count):
    half_dim = HD // 2
    frequency = 10000.0 ** (-jnp.arange(half_dim, dtype=jnp.float32) / half_dim)
    angle_table = jnp.arange(row_count, dtype=jnp.float32)[:, None] * frequency[None, :]
    return (jnp.cos(angle_table), jnp.sin(angle_table))


def rotate(vectors, cosine_table, sine_table):
    half_dim = vectors.shape[-1] // 2
    first_half = vectors[..., :half_dim]
    second_half = vectors[..., half_dim:]
    cosine_b = cosine_table[:, None, :]
    sine_b = sine_table[:, None, :]
    return jnp.concatenate(
        [
            first_half * cosine_b - second_half * sine_b,
            second_half * cosine_b + first_half * sine_b,
        ],
        axis=-1,
    )


def unrotate(vectors, cosine_table, sine_table):
    half_dim = vectors.shape[-1] // 2
    first_half = vectors[..., :half_dim]
    second_half = vectors[..., half_dim:]
    cosine_b = cosine_table[:, None, :]
    sine_b = sine_table[:, None, :]
    return jnp.concatenate(
        [
            first_half * cosine_b + second_half * sine_b,
            second_half * cosine_b - first_half * sine_b,
        ],
        axis=-1,
    )


def transpose_product(grad_low, matrix):
    return lax.dot_general(
        grad_low, matrix, (((1,), (1,)), ((), ())), preferred_element_type=jnp.float32
    )


def attention_window(full_rows, gain, w_query, w_key, w_value, cotangent, valid_rows, prompt_len):
    batch_size, row_count, model_width = full_rows.shape
    head_count = w_query.shape[1] // HD
    wide_rows = full_rows.astype(jnp.float32)
    inv_rms = lax.rsqrt(jnp.mean(wide_rows * wide_rows, axis=-1) + 1e-05)
    normed = (
        (wide_rows * inv_rms[..., None] * gain)
        .astype(jnp.bfloat16)
        .reshape(batch_size * row_count, model_width)
    )
    cosine_table, sine_table = rope_tables(row_count)

    def project(matrix):
        return jnp.dot(normed, matrix, preferred_element_type=jnp.float32).reshape(
            batch_size, row_count, head_count, HD
        )

    queries = rotate(project(w_query), cosine_table, sine_table).astype(jnp.bfloat16)
    key_rows = rotate(project(w_key), cosine_table, sine_table).astype(jnp.bfloat16)
    value_rows = project(w_value).astype(jnp.bfloat16)
    score_scale = 1.0 / math.sqrt(HD)
    scores = (
        jnp.einsum("erhd,ekhd->ehrk", queries, key_rows, preferred_element_type=jnp.float32)
        * score_scale
    )
    rows_at = jnp.arange(row_count, dtype=jnp.int32)
    row_limit = prompt_len + valid_rows
    allowed = (rows_at[None, None, :] <= rows_at[None, :, None]) & (
        rows_at[None, None, :] < row_limit[:, None, None]
    )
    allowed = allowed[:, None]
    scores = jnp.where(allowed, scores, -1e30)
    row_peak = jnp.max(scores, axis=-1, keepdims=True)
    weights = jnp.where(allowed, jnp.exp(scores - row_peak), 0.0)
    probability = weights / jnp.sum(weights, axis=-1, keepdims=True)
    probs_low = probability.astype(jnp.bfloat16)
    live_rows = rows_at[None, :] < row_limit[:, None]
    mixed_rows = jnp.einsum(
        "ehrk,ekhd->erhd", probs_low, value_rows, preferred_element_type=jnp.float32
    )
    mixed_rows = jnp.where(live_rows[:, :, None, None], mixed_rows, 0.0)
    output = mixed_rows.reshape(batch_size, row_count, head_count * HD).astype(jnp.bfloat16)
    upstream = jnp.where(
        live_rows[:, :, None, None], cotangent.reshape(batch_size, row_count, head_count, HD), 0.0
    )
    grad_prob = jnp.einsum(
        "erhd,ekhd->ehrk", upstream, value_rows, preferred_element_type=jnp.float32
    )
    row_delta = jnp.sum(probability * grad_prob, axis=-1, keepdims=True)
    grad_score = (probability * (grad_prob - row_delta)).astype(jnp.bfloat16)
    grad_query = (
        jnp.einsum(
            "ehrk,ekhd->erhd",
            grad_score[:, :, :prompt_len, :],
            key_rows,
            preferred_element_type=jnp.float32,
        )
        * score_scale
    )
    grad_key = (
        jnp.einsum(
            "ehrk,erhd->ekhd",
            grad_score[:, :, :, :prompt_len],
            queries,
            preferred_element_type=jnp.float32,
        )
        * score_scale
    )
    grad_value = jnp.einsum(
        "ehrk,erhd->ekhd",
        probs_low[:, :, :, :prompt_len],
        upstream,
        preferred_element_type=jnp.float32,
    )
    cosine_lead = cosine_table[:prompt_len]
    sine_lead = sine_table[:prompt_len]
    flat_rows = batch_size * prompt_len
    grad_query = (
        unrotate(grad_query, cosine_lead, sine_lead)
        .astype(jnp.bfloat16)
        .reshape(flat_rows, head_count * HD)
    )
    grad_key = (
        unrotate(grad_key, cosine_lead, sine_lead)
        .astype(jnp.bfloat16)
        .reshape(flat_rows, head_count * HD)
    )
    grad_value = grad_value.astype(jnp.bfloat16).reshape(flat_rows, head_count * HD)
    grad_normed = (
        transpose_product(grad_query, w_query)
        + transpose_product(grad_key, w_key)
        + transpose_product(grad_value, w_value)
    )
    grad_normed = grad_normed.reshape(batch_size, prompt_len, model_width) * gain
    prompt_rows = wide_rows[:, :prompt_len]
    prompt_inv = inv_rms[:, :prompt_len, None]
    grad_rows = prompt_inv * grad_normed - prompt_rows * prompt_inv**3 * jnp.mean(
        grad_normed * prompt_rows, axis=-1, keepdims=True
    )
    return (output, grad_rows)


def on_device(text, prompts, gain, w_query, w_key, w_value, cotangent, task_of, lengths, slot):
    dp_count = lax.axis_size("dp")
    my_index = lax.axis_index("dp")
    ex_dev = text.shape[0]
    task_dev = prompts.shape[0]
    prompt_len = prompts.shape[1]
    example_count = slot.shape[0]
    task_count = task_dev * dp_count
    places = jnp.arange(example_count, dtype=jnp.int32)
    matching = slot[None, :] == places[:, None]
    task_slot = jnp.sum(jnp.where(matching, task_of[None, :], 0), axis=1)
    length_slot = jnp.sum(jnp.where(matching, lengths[None, :], 0), axis=1)
    first_place = my_index * ex_dev
    my_lengths = lax.dynamic_slice_in_dim(length_slot, first_place, ex_dev)
    task_ids = jnp.arange(task_count, dtype=jnp.int32)
    spread_text, spread_prompts = (
        lax.all_to_all(text, "dp", split_axis=2, concat_axis=0, tiled=True),
        lax.all_to_all(prompts, "dp", split_axis=2, concat_axis=0, tiled=True),
    )
    taking = matching.astype(jnp.bfloat16)
    placed_text = jnp.einsum(
        "se,erc->src", taking, spread_text, preferred_element_type=jnp.bfloat16
    )
    choosing = (task_slot[:, None] == task_ids[None, :]).astype(jnp.bfloat16)
    placed_prompts = jnp.einsum(
        "st,tpc->spc", choosing, spread_prompts, preferred_element_type=jnp.bfloat16
    )
    placed = jnp.concatenate([placed_prompts, placed_text], axis=1)
    placed = placed.reshape(dp_count, ex_dev, placed.shape[1], placed.shape[2])
    local_rows = lax.all_to_all(placed, "dp", split_axis=0, concat_axis=3, tiled=True)[0]
    full_rows = lax.all_gather(local_rows, "tensor", axis=2, tiled=True)
    output, grad_part = attention_window(
        full_rows, gain, w_query, w_key, w_value, cotangent, my_lengths, prompt_len
    )
    grad_share = lax.psum_scatter(grad_part, "tensor", scatter_dimension=2, tiled=True)
    spread_grads = lax.all_to_all(grad_share, "dp", split_axis=2, concat_axis=0, tiled=True)
    collecting = (task_ids[:, None] == task_slot[None, :]).astype(jnp.float32)
    per_task = jnp.einsum("ts,spc->tpc", collecting, spread_grads, precision=lax.Precision.HIGHEST)
    prompt_grad = lax.all_to_all(per_task, "dp", split_axis=0, concat_axis=2, tiled=True)
    return (output, prompt_grad)


MESH = pl.DeviceIdType.MESH
PAD_POS = 1 << 20
TILE = 8


def dot_nn(a, b):
    return jnp.dot(a, b, preferred_element_type=jnp.float32)


def dot_nt(a, b):
    return lax.dot_general(a, b, (((1,), (1,)), ((), ())), preferred_element_type=jnp.float32)


def dot_tn(a, b):
    return lax.dot_general(a, b, (((0,), (0,)), ((), ())), preferred_element_type=jnp.float32)


def partner(me, k):
    bit, peer = 1, me
    while bit <= k:
        if k & bit:
            peer = peer + bit - 2 * bit * lax.rem(me // bit, 2)
        bit *= 2
    return peer


def origin_table(m):
    table = []
    for t in range(m):
        others = [z for z in range(m) if z != t]
        others.sort(key=lambda z: (abs(z - t), (z < t) == (2 * t < m)))
        table.append(others)
    return table


def step_kernel(
    p_len, slot_ref, task_ref, length_ref, text_ref, prompts_ref, gain_ref, cos_ref, sin_ref,
    cot_ref, wq_hbm, wk_hbm, wv_hbm, out_ref, grad_ref,
    w_ref, pbuf, precv, psend, fullp, tz, stage, tsend, fullt, squares, qkv, grads, inv_ref, cot_pad,
    part, pin, send4, gout,
    semw, sem_t, sem_p, sem_c, sem_s, semz_own, semz_fwd, semz_in, semq, semg, semg_in, sem4,
):
    n, m = lax.axis_size("dp"), lax.axis_size("tensor")
    me, t = lax.axis_index("dp"), lax.axis_index("tensor")
    f32, bf16 = jnp.float32, jnp.bfloat16
    tu, _, _, width = text_ref.shape
    blocks, model_width, group = w_ref.shape
    per = blocks // 3
    pt = -(-p_len // TILE)
    pu = -(-pt // n)
    lead = pt * TILE
    seq = tu * n * TILE
    rows = lead + seq
    counts = [min(n, pt - v * n) for v in range(pu)]
    peers = [partner(me, k) for k in range(n)]
    table = origin_table(m)

    def pick(place, values):
        total = jnp.int32(0)
        for e in range(n):
            total = jnp.maximum(total, jnp.where(slot_ref[e] == place, values(e), 0))
        return total

    def by_place(values):
        total = jnp.int32(0)
        for z in range(m):
            total = total + jnp.where(t == z, values[z], 0)
        return total

    origins = [by_place([table[z][i] for z in range(m)]) for i in range(m - 1)]

    def describe(src, dst, send, recv, device):
        return pltpu.make_async_remote_copy(
            src_ref=src,
            dst_ref=dst,
            send_sem=send,
            recv_sem=recv,
            device_id=device,
            device_id_type=MESH,
        )

    waits = []

    def remote(src, dst, send, recv, device, needed=None):
        copy = describe(src, dst, send, recv, device)
        if needed is None:
            copy.start()
        else:
            pl.when(needed)(copy.start)
        waits.append((copy, needed))
        return copy

    loads = []
    for i, hbm in enumerate((wq_hbm, wk_hbm, wv_hbm)):
        for g in range(per):
            at = i * per + g
            load = pltpu.make_async_copy(
                hbm.at[:, g * group : (g + 1) * group], w_ref.at[at], semw.at[at]
            )
            load.start()
            loads.append(load)

    barrier = pltpu.get_barrier_semaphore()
    for z in range(m):
        for k in range(n):
            far = lax.rem(t + z, m)
            if z or k:
                pl.semaphore_signal(
                    barrier, inc=1, device_id=(peers[k], far), device_id_type=MESH
                )

    whole = p_len // TILE
    pbuf[:whole] = prompts_ref[: whole * TILE].reshape(whole, TILE, width)
    if p_len % TILE:
        rest = prompts_ref[whole * TILE : p_len].astype(f32)
        fill = jnp.zeros((TILE - p_len % TILE, width), f32)
        pbuf[whole] = jnp.concatenate([rest, fill], axis=0).astype(bf16)
    if pu * n > pt:
        pbuf[pt:] = jnp.zeros((pu * n - pt, TILE, width), bf16)
    cot_pad[:lead] = cot_ref[:lead]
    cot_pad[lead:] = cot_ref[p_len:].astype(f32).astype(bf16)
    pl.semaphore_wait(barrier, n * m - 1)

    spread_0, spread_t, spread_p = [], [], []
    for k in range(1, n):
        spread_0.append(
            remote(
                text_ref.at[0, peers[k]], tz.at[t, 0, me],
                sem_t.at[0, 0, k], sem_t.at[1, 0, k], (peers[k], t),
            )
        )
    for k in range(1, n):
        if tu > 1:
            spread_t.append(
                remote(
                    text_ref.at[1:, peers[k]], tz.at[t, 1:, me],
                    sem_t.at[0, 1, k], sem_t.at[1, 1, k], (peers[k], t),
                )
            )
    for k in range(1, n):
        for v in range(pu):
            spread_p.append(
                remote(
                    pbuf.at[v * n + peers[k]], precv.at[v, me],
                    sem_p.at[0, v, k], sem_p.at[1, v, k], (peers[k], t),
                )
            )
    for u in range(tu):
        tz[t, u, me] = text_ref[u, me]
    for v in range(pu):
        precv[v, me] = pbuf[v * n + me]

    ways = [(t < m - 1, lax.rem(t + 1, m)), (t > 0, lax.rem(t + m - 1, m))]

    def text_unit(z, g):
        return tz.at[z, g]

    def prompt_unit(z, v):
        return fullp.at[z, v, : counts[v]]

    units = [(text_unit, g) for g in range(tu)] + [(prompt_unit, v) for v in range(pu)]

    def pass_own(i):
        ref = units[i][0](t, units[i][1])
        for w, (needed, far) in enumerate(ways):
            remote(ref, ref, semz_own.at[w, i], semz_in.at[t, i], (me, far), needed)

    for copy in spread_0:
        copy.wait_recv()
    pass_own(0)
    for copy in spread_t:
        copy.wait_recv()
    for g in range(1, tu):
        pass_own(g)

    sources = [pick(peers[k], lambda e: e) for k in range(n)]
    tasks_of = [pick(peers[k], lambda e: task_ref[e]) for k in range(n)]

    for copy in spread_p:
        copy.wait_recv()
    collect_p = []
    for k in range(1, n):
        for v in range(pu):
            psend[k, v] = precv[v, tasks_of[k]]
        collect_p.append(
            remote(
                psend.at[k], fullp.at[t, :, me], sem_c.at[0, k], sem_c.at[1, k], (peers[k], t)
            )
        )
    for v in range(pu):
        fullp[t, v, me] = precv[v, tasks_of[0]]
    collected = {}

    def collect(i, z, lo, hi):
        for u in range(lo, hi):
            stage[u - lo] = tz[z, u]
        for k in range(1, n):
            for u in range(lo, hi):
                tsend[i, k, u] = stage[u - lo, sources[k]]
            collected[i, lo, k] = remote(
                tsend.at[i, k, lo:hi], fullt.at[z, lo:hi, me],
                sem_s.at[0, i, lo, k], sem_s.at[1, i, lo, k], (peers[k], t),
            )
        for u in range(lo, hi):
            fullt[z, u, me] = stage[u - lo, sources[0]]

    def finish(i):
        for key, copy in collected.items():
            if key[0] == i:
                copy.wait_recv()

    collect(m - 1, t, 0, tu)
    for copy in collect_p:
        copy.wait_recv()
    for v in range(pu):
        pass_own(tu + v)
    finish(m - 1)

    def whole_rows(z):
        prompt = fullp[z].reshape(pu * n * TILE, width)[:lead]
        return jnp.concatenate([prompt, fullt[z].reshape(seq, width)], axis=0)

    own = whole_rows(t).astype(f32)
    square = jnp.broadcast_to(jnp.sum(own * own, axis=1, keepdims=True), (rows, 128))
    padded = squares.shape[2]
    square = jnp.concatenate([square, jnp.zeros((padded - rows, 128), f32)], axis=0)
    squares[0] = square.T[:8]
    shared = []
    for k in range(1, m):
        shared.append(
            remote(
                squares.at[0], squares.at[k], semq.at[0, k], semq.at[1, k],
                (me, lax.rem(t + k, m)),
            )
        )

    def project(z, fresh):
        wide = whole_rows(z).astype(f32)
        normed = (wide * inv_ref[:, :1] * gain_ref[z]).astype(bf16)
        deep = pl.ds(pl.multiple_of(z * width, width), width)

        def body(b, carry):
            product = dot_nn(normed, w_ref[b, deep, :])
            qkv[b] = product if fresh else qkv[b] + product
            return carry

        lax.fori_loop(0, blocks, body, 0)

    def receive(i):
        z = origins[i]
        left = z < t
        needed = (left & (t < m - 1)) | (jnp.logical_not(left) & (t > 0))
        far = jnp.where(needed, jnp.where(left, t + 1, t - 1), z)
        step = 1 if i == m - 2 else max(1, tu // 2)
        for j, (unit, g) in enumerate(units):
            ref = unit(z, g)
            describe(ref, ref, semz_fwd.at[i, j], semz_in.at[z, j], (me, far)).wait_recv()
            remote(ref, ref, semz_fwd.at[i, j], semz_in.at[z, j], (me, far), needed)
            if j < tu and (j + 1) % step == 0:
                collect(i, z, j + 1 - step, j + 1)
        finish(i)

    receive(0)
    for copy in shared:
        copy.wait_recv()
    square = squares[0]
    for k in range(1, m):
        square = square + squares[k]
    square = jnp.broadcast_to(square[:1], (128, padded)).T[:rows]
    inv_ref[...] = lax.rsqrt(square * (1.0 / model_width) + 1e-05)
    for load in loads:
        load.wait()
    project(t, True)
    project(origins[0], False)
    for i in range(1, m - 1):
        receive(i)
        project(origins[i], False)

    limit = p_len + pick(me, lambda e: length_ref[e])
    scale = 1.0 / math.sqrt(HD)

    def positions(shape, axis):
        at = lax.broadcasted_iota(jnp.int32, shape, axis)
        return jnp.where(at < lead, jnp.where(at < p_len, at, PAD_POS), at - (lead - p_len))

    def heads(g, dots):
        cosine, sine = cos_ref[...], sin_ref[...]
        cosine_p, sine_p = cosine[:lead], sine[:lead]
        row_pos = positions((rows, 1), 0)
        col_pos = positions((1, rows), 1)
        allowed = (col_pos <= row_pos) & (col_pos < limit)
        live = row_pos < limit
        edge = min(rows, -(-lead // 128) * 128)
        for h in range(group // HD):
            at = slice(h * HD, (h + 1) * HD)
            far = pl.ds(pl.multiple_of(g * group + h * HD, HD), HD)
            q_raw, k_raw, v_raw = qkv[g, :, at], qkv[per + g, :, at], qkv[2 * per + g, :, at]
            v = v_raw.astype(bf16)
            q = (q_raw * cosine + pltpu.roll(q_raw, HD // 2, 1) * sine).astype(bf16)
            k = (k_raw * cosine + pltpu.roll(k_raw, HD // 2, 1) * sine).astype(bf16)
            scores = jnp.where(allowed, dot_nt(q, k) * scale, -1e30)
            peak = jnp.max(scores, axis=1, keepdims=True)
            weights = jnp.exp(scores - peak)
            probs = weights * (1.0 / jnp.sum(weights, axis=1, keepdims=True))
            low = probs.astype(bf16)
            out_ref[:, far] = jnp.where(live, dot_nn(low, v), 0.0).astype(bf16)
            upstream = jnp.where(live, cot_pad[:, far].astype(f32), 0.0).astype(bf16)
            grad_prob = dot_nt(upstream, v)
            delta = jnp.sum(probs * grad_prob, axis=1, keepdims=True)
            grad_score = (probs * (grad_prob - delta)).astype(bf16)
            gq = dot_nn(grad_score[:lead, :edge], k[:edge]) * scale
            gk = dot_tn(grad_score[:, :edge], q)[:lead] * scale
            gv = dot_tn(low[:, :edge], upstream)[:lead]
            gq = (gq * cosine_p - pltpu.roll(gq, HD // 2, 1) * sine_p).astype(bf16)
            gk = (gk * cosine_p - pltpu.roll(gk, HD // 2, 1) * sine_p).astype(bf16)
            gv = gv.astype(bf16)
            grads[g, :, at] = gq
            grads[per + g, :, at] = gk
            grads[2 * per + g, :, at] = gv
            along = gq.astype(f32) * q_raw[:lead] + gk.astype(f32) * k_raw[:lead]
            along = along + gv.astype(f32) * v_raw[:lead]
            dots = dots + jnp.sum(along, axis=1, keepdims=True)
        return dots

    dots = lax.fori_loop(0, per, heads, jnp.zeros((lead, 1), f32))
    inv = inv_ref[:lead, :1]
    factor = inv * inv * (dots * (1.0 / model_width))

    def holds(v, at):
        return None if counts[v] == n else v * n + at < pt

    def when(needed, act):
        if needed is None:
            act()
        else:
            pl.when(needed)(act)

    for i in range(m):
        z = origins[m - 2 - i] if i < m - 1 else t
        deep = pl.ds(pl.multiple_of(z * width, width), width)
        total = dot_nt(grads[0], w_ref[0, deep, :])
        for b in range(1, blocks):
            total = total + dot_nt(grads[b], w_ref[b, deep, :])
        prompt = fullp[z].reshape(pu * n * TILE, width)[:lead].astype(f32)
        value = inv * (total * gain_ref[z]) - prompt * factor
        part[i, :pt] = value.astype(bf16).reshape(pt, TILE, width)
        for k in range(n):
            for v in range(pu):
                if i == m - 1 and k == 0:
                    continue
                remote(
                    part.at[i, v * n + peers[k]], pin.at[v, me, t],
                    semg.at[i, v, k], semg_in.at[v, k, t], (peers[k], z), holds(v, peers[k]),
                )
        if i == m - 1:
            for v in range(pu):

                def keep(v=v):
                    pin[v, me, t] = part[m - 1, v * n + me]

                when(holds(v, me), keep)

    tasks = [pick(s, lambda e: task_ref[e]) for s in range(n)]
    fourth = {}
    for v in range(pu):

        def gather(v=v):
            for k in range(n):
                for z in range(m):
                    spot = lax.rem(t + z, m)
                    if k or z:
                        describe(
                            pin.at[v, peers[k], spot], pin.at[v, peers[k], spot],
                            semg.at[0, v, k], semg_in.at[v, k, spot], (peers[k], spot),
                        ).wait_recv()
            for s in range(n):
                total = pin[v, s, 0].astype(f32)
                for z in range(1, m):
                    total = total + pin[v, s, z].astype(f32)
                for k in range(n):
                    hit = jnp.where(tasks[s] == peers[k], total, 0.0)
                    sums[k] = hit if s == 0 else sums[k] + hit
            for k in range(n):
                if k == 0:
                    gout[v, me] = sums[k].astype(bf16)
                else:
                    send4[v, k] = sums[k].astype(bf16)

        sums = [None] * n
        when(holds(v, me), gather)
        for k in range(1, n):
            fourth[v, k] = remote(
                send4.at[v, k], gout.at[v, me], sem4.at[0, v, k], sem4.at[1, v, k],
                (peers[k], t), holds(v, me),
            )
    for v in range(pu):
        for k in range(1, n):
            when(holds(v, peers[k]), fourth[v, k].wait_recv)
        grad_ref[v * n : v * n + counts[v]] = gout[v, : counts[v]]
    for copy, needed in waits:
        when(needed, copy.wait_send)


def fast_device(text, prompts, gain, w_query, w_key, w_value, cotangent, task_of, lengths, slot):
    n, m = lax.axis_size("dp"), lax.axis_size("tensor")
    f32, bf16 = jnp.float32, jnp.bfloat16
    seq, width = text.shape[1], text.shape[2]
    p_len = prompts.shape[1]
    heads = w_query.shape[1]
    tu = seq // (TILE * n)
    pt = -(-p_len // TILE)
    pu = -(-pt // n)
    lead = pt * TILE
    rows = lead + seq
    row = np.arange(rows)
    pos = np.where(row < lead, np.where(row < p_len, row, 0), row - (lead - p_len))
    half = HD // 2
    frequency = 10000.0 ** (-jnp.arange(half, dtype=f32) / half)
    angle = jnp.asarray(pos.astype(np.int32)).astype(f32)[:, None] * frequency[None, :]
    cosine = jnp.concatenate([jnp.cos(angle)] * 2, axis=1)
    sine = jnp.concatenate([-jnp.sin(angle), jnp.sin(angle)], axis=1)
    group = 2 * HD if heads % (2 * HD) == 0 else HD
    blocks = 3 * (heads // group)
    units = tu + pu
    smem = pl.BlockSpec(memory_space=pltpu.SMEM)
    vmem = pl.BlockSpec(memory_space=pltpu.VMEM)
    hbm = pl.BlockSpec(memory_space=pl.ANY)
    dma = pltpu.SemaphoreType.DMA
    out, collected = pl.pallas_call(
        functools.partial(step_kernel, p_len),
        out_shape=(
            jax.ShapeDtypeStruct((rows, heads), bf16),
            jax.ShapeDtypeStruct((pt, TILE, width), bf16),
        ),
        in_specs=[smem] * 3 + [vmem] * 6 + [hbm] * 3,
        out_specs=(vmem, vmem),
        scratch_shapes=[
            pltpu.VMEM((blocks, m * width, group), bf16),
            pltpu.VMEM((pu * n, TILE, width), bf16),
            pltpu.VMEM((pu, n, TILE, width), bf16),
            pltpu.VMEM((n, pu, TILE, width), bf16),
            pltpu.VMEM((m, pu, n, TILE, width), bf16),
            pltpu.VMEM((m, tu, n, TILE, width), bf16),
            pltpu.VMEM((tu, n, TILE, width), bf16),
            pltpu.VMEM((m, n, tu, TILE, width), bf16),
            pltpu.VMEM((m, tu, n, TILE, width), bf16),
            pltpu.VMEM((m, 8, -(-rows // 128) * 128), f32),
            pltpu.VMEM((blocks, rows, group), f32),
            pltpu.VMEM((blocks, lead, group), bf16),
            pltpu.VMEM((rows, 128), f32),
            pltpu.VMEM((rows, heads), bf16),
            pltpu.VMEM((m, pu * n, TILE, width), bf16),
            pltpu.VMEM((pu, n, m, TILE, width), bf16),
            pltpu.VMEM((pu, n, TILE, width), bf16),
            pltpu.VMEM((pu, n, TILE, width), bf16),
            dma((blocks,)),
            dma((2, 2, n)),
            dma((2, pu, n)),
            dma((2, n)),
            dma((2, m, tu, n)),
            dma((2, units)),
            dma((m, units)),
            dma((m, units)),
            dma((2, m)),
            dma((m, pu, n)),
            dma((pu, n, m)),
            dma((2, pu, n)),
        ],
        compiler_params=pltpu.CompilerParams(
            collective_id=0, has_side_effects=True, vmem_limit_bytes=63 * 2**20
        ),
    )(
        slot, task_of, lengths, text.reshape(tu, n, TILE, width), prompts[0],
        gain.reshape(m, 1, width), cosine, sine, cotangent[0], w_query, w_key, w_value,
    )
    prompt_grad = collected.reshape(lead, width)[:p_len].astype(f32)[None]
    attn_out = jnp.concatenate([out[:p_len], out[lead:]], axis=0)[None]
    return (attn_out, prompt_grad)


def choose(text, prompts, *rest):
    n, m = lax.axis_size("dp"), lax.axis_size("tensor")
    seq, p_len = text.shape[1], prompts.shape[1]
    fits = (
        text.shape[0] == 1
        and prompts.shape[0] == 1
        and m >= 2
        and n >= 2
        and n & (n - 1) == 0
        and n <= 8
        and seq % (TILE * n) == 0
        and text.shape[2] % 128 == 0
    )
    return (fast_device if fits else on_device)(text, prompts, *rest)


def solution(mesh):
    in_specs = (
        P("dp", None, "tensor"),
        P("dp", None, "tensor"),
        P(),
        P(None, "tensor"),
        P(None, "tensor"),
        P(None, "tensor"),
        P("dp", None, "tensor"),
        P(),
        P(),
        P(),
    )
    out_specs = (P("dp", None, "tensor"), P("dp", None, "tensor"))
    return jax.shard_map(
        choose, mesh=mesh, in_specs=in_specs, out_specs=out_specs, check_vma=False
    )
```

```python
import functools
import math

import jax
import jax.numpy as jnp
import numpy as np
from jax import lax
from jax.experimental import pallas as pl
from jax.experimental.pallas import tpu as pltpu
from jax.sharding import PartitionSpec as P

HD = 128


def rope_tables(row_count):
    half_dim = HD // 2
    frequency = 10000.0 ** (-jnp.arange(half_dim, dtype=jnp.float32) / half_dim)
    angle_table = jnp.arange(row_count, dtype=jnp.float32)[:, None] * frequency[None, :]
    return (jnp.cos(angle_table), jnp.sin(angle_table))


def rotate(vectors, cosine_table, sine_table):
    half_dim = vectors.shape[-1] // 2
    first_half = vectors[..., :half_dim]
    second_half = vectors[..., half_dim:]
    cosine_b = cosine_table[:, None, :]
    sine_b = sine_table[:, None, :]
    return jnp.concatenate(
        [
            first_half * cosine_b - second_half * sine_b,
            second_half * cosine_b + first_half * sine_b,
        ],
        axis=-1,
    )


def unrotate(vectors, cosine_table, sine_table):
    half_dim = vectors.shape[-1] // 2
    first_half = vectors[..., :half_dim]
    second_half = vectors[..., half_dim:]
    cosine_b = cosine_table[:, None, :]
    sine_b = sine_table[:, None, :]
    return jnp.concatenate(
        [
            first_half * cosine_b + second_half * sine_b,
            second_half * cosine_b - first_half * sine_b,
        ],
        axis=-1,
    )


def transpose_product(grad_low, matrix):
    return lax.dot_general(
        grad_low, matrix, (((1,), (1,)), ((), ())), preferred_element_type=jnp.float32
    )


def attention_window(full_rows, gain, w_query, w_key, w_value, cotangent, valid_rows, prompt_len):
    batch_size, row_count, model_width = full_rows.shape
    head_count = w_query.shape[1] // HD
    wide_rows = full_rows.astype(jnp.float32)
    inv_rms = lax.rsqrt(jnp.mean(wide_rows * wide_rows, axis=-1) + 1e-05)
    normed = (
        (wide_rows * inv_rms[..., None] * gain)
        .astype(jnp.bfloat16)
        .reshape(batch_size * row_count, model_width)
    )
    cosine_table, sine_table = rope_tables(row_count)

    def project(matrix):
        return jnp.dot(normed, matrix, preferred_element_type=jnp.float32).reshape(
            batch_size, row_count, head_count, HD
        )

    queries = rotate(project(w_query), cosine_table, sine_table).astype(jnp.bfloat16)
    key_rows = rotate(project(w_key), cosine_table, sine_table).astype(jnp.bfloat16)
    value_rows = project(w_value).astype(jnp.bfloat16)
    score_scale = 1.0 / math.sqrt(HD)
    scores = (
        jnp.einsum("erhd,ekhd->ehrk", queries, key_rows, preferred_element_type=jnp.float32)
        * score_scale
    )
    rows_at = jnp.arange(row_count, dtype=jnp.int32)
    row_limit = prompt_len + valid_rows
    allowed = (rows_at[None, None, :] <= rows_at[None, :, None]) & (
        rows_at[None, None, :] < row_limit[:, None, None]
    )
    allowed = allowed[:, None]
    scores = jnp.where(allowed, scores, -1e30)
    row_peak = jnp.max(scores, axis=-1, keepdims=True)
    weights = jnp.where(allowed, jnp.exp(scores - row_peak), 0.0)
    probability = weights / jnp.sum(weights, axis=-1, keepdims=True)
    probs_low = probability.astype(jnp.bfloat16)
    live_rows = rows_at[None, :] < row_limit[:, None]
    mixed_rows = jnp.einsum(
        "ehrk,ekhd->erhd", probs_low, value_rows, preferred_element_type=jnp.float32
    )
    mixed_rows = jnp.where(live_rows[:, :, None, None], mixed_rows, 0.0)
    output = mixed_rows.reshape(batch_size, row_count, head_count * HD).astype(jnp.bfloat16)
    upstream = jnp.where(
        live_rows[:, :, None, None], cotangent.reshape(batch_size, row_count, head_count, HD), 0.0
    )
    grad_prob = jnp.einsum(
        "erhd,ekhd->ehrk", upstream, value_rows, preferred_element_type=jnp.float32
    )
    row_delta = jnp.sum(probability * grad_prob, axis=-1, keepdims=True)
    grad_score = (probability * (grad_prob - row_delta)).astype(jnp.bfloat16)
    grad_query = (
        jnp.einsum(
            "ehrk,ekhd->erhd",
            grad_score[:, :, :prompt_len, :],
            key_rows,
            preferred_element_type=jnp.float32,
        )
        * score_scale
    )
    grad_key = (
        jnp.einsum(
            "ehrk,erhd->ekhd",
            grad_score[:, :, :, :prompt_len],
            queries,
            preferred_element_type=jnp.float32,
        )
        * score_scale
    )
    grad_value = jnp.einsum(
        "ehrk,erhd->ekhd",
        probs_low[:, :, :, :prompt_len],
        upstream,
        preferred_element_type=jnp.float32,
    )
    cosine_lead = cosine_table[:prompt_len]
    sine_lead = sine_table[:prompt_len]
    flat_rows = batch_size * prompt_len
    grad_query = (
        unrotate(grad_query, cosine_lead, sine_lead)
        .astype(jnp.bfloat16)
        .reshape(flat_rows, head_count * HD)
    )
    grad_key = (
        unrotate(grad_key, cosine_lead, sine_lead)
        .astype(jnp.bfloat16)
        .reshape(flat_rows, head_count * HD)
    )
    grad_value = grad_value.astype(jnp.bfloat16).reshape(flat_rows, head_count * HD)
    grad_normed = (
        transpose_product(grad_query, w_query)
        + transpose_product(grad_key, w_key)
        + transpose_product(grad_value, w_value)
    )
    grad_normed = grad_normed.reshape(batch_size, prompt_len, model_width) * gain
    prompt_rows = wide_rows[:, :prompt_len]
    prompt_inv = inv_rms[:, :prompt_len, None]
    grad_rows = prompt_inv * grad_normed - prompt_rows * prompt_inv**3 * jnp.mean(
        grad_normed * prompt_rows, axis=-1, keepdims=True
    )
    return (output, grad_rows)


def on_device(text, prompts, gain, w_query, w_key, w_value, cotangent, task_of, lengths, slot):
    dp_count = lax.axis_size("dp")
    my_index = lax.axis_index("dp")
    ex_dev = text.shape[0]
    task_dev = prompts.shape[0]
    prompt_len = prompts.shape[1]
    example_count = slot.shape[0]
    task_count = task_dev * dp_count
    places = jnp.arange(example_count, dtype=jnp.int32)
    matching = slot[None, :] == places[:, None]
    task_slot = jnp.sum(jnp.where(matching, task_of[None, :], 0), axis=1)
    length_slot = jnp.sum(jnp.where(matching, lengths[None, :], 0), axis=1)
    first_place = my_index * ex_dev
    my_lengths = lax.dynamic_slice_in_dim(length_slot, first_place, ex_dev)
    task_ids = jnp.arange(task_count, dtype=jnp.int32)
    spread_text, spread_prompts = (
        lax.all_to_all(text, "dp", split_axis=2, concat_axis=0, tiled=True),
        lax.all_to_all(prompts, "dp", split_axis=2, concat_axis=0, tiled=True),
    )
    taking = matching.astype(jnp.bfloat16)
    placed_text = jnp.einsum(
        "se,erc->src", taking, spread_text, preferred_element_type=jnp.bfloat16
    )
    choosing = (task_slot[:, None] == task_ids[None, :]).astype(jnp.bfloat16)
    placed_prompts = jnp.einsum(
        "st,tpc->spc", choosing, spread_prompts, preferred_element_type=jnp.bfloat16
    )
    placed = jnp.concatenate([placed_prompts, placed_text], axis=1)
    placed = placed.reshape(dp_count, ex_dev, placed.shape[1], placed.shape[2])
    local_rows = lax.all_to_all(placed, "dp", split_axis=0, concat_axis=3, tiled=True)[0]
    full_rows = lax.all_gather(local_rows, "tensor", axis=2, tiled=True)
    output, grad_part = attention_window(
        full_rows, gain, w_query, w_key, w_value, cotangent, my_lengths, prompt_len
    )
    grad_share = lax.psum_scatter(grad_part, "tensor", scatter_dimension=2, tiled=True)
    spread_grads = lax.all_to_all(grad_share, "dp", split_axis=2, concat_axis=0, tiled=True)
    collecting = (task_ids[:, None] == task_slot[None, :]).astype(jnp.float32)
    per_task = jnp.einsum("ts,spc->tpc", collecting, spread_grads, precision=lax.Precision.HIGHEST)
    prompt_grad = lax.all_to_all(per_task, "dp", split_axis=0, concat_axis=2, tiled=True)
    return (output, prompt_grad)


MESH = pl.DeviceIdType.MESH
PAD_POS = 1 << 20
TILE = 8


def dot_nn(a, b):
    return jnp.dot(a, b, preferred_element_type=jnp.float32)


def dot_nt(a, b):
    return lax.dot_general(a, b, (((1,), (1,)), ((), ())), preferred_element_type=jnp.float32)


def dot_tn(a, b):
    return lax.dot_general(a, b, (((0,), (0,)), ((), ())), preferred_element_type=jnp.float32)


def partner(me, k):
    bit, peer = 1, me
    while bit <= k:
        if k & bit:
            peer = peer + bit - 2 * bit * lax.rem(me // bit, 2)
        bit *= 2
    return peer


def origin_table(m):
    table = []
    for t in range(m):
        others = [z for z in range(m) if z != t]
        others.sort(key=lambda z: (abs(z - t), (z < t) == (2 * t < m)))
        table.append(others)
    return table


def step_kernel(
    p_len, slots, slot_ref, task_ref, length_ref, text_hbm, prompts_hbm, gain_hbm, cos_hbm, sin_hbm,
    cot_hbm, wq_hbm, wk_hbm, wv_hbm, out_ref, grad_ref,
    w_ref, text_ref, prompts_ref, gain_ref, cos_ref, sin_ref, cot_ref,
    pbuf, precv, psend, fullp, trecv, tz, stage, tsend, fullt, squares, qkv, grads, inv_ref, cot_pad,
    part, pin, send4, gout,
    semw, semi, sem_t, sem_p, sem_c, sem_s, semz_own, semz_fwd, semz_in, semq, semg, semg_in, sem4,
):
    n, m = lax.axis_size("dp"), lax.axis_size("tensor")
    me, t = lax.axis_index("dp"), lax.axis_index("tensor")
    f32, bf16 = jnp.float32, jnp.bfloat16
    tu, _, _, width = text_ref.shape
    blocks, model_width, group = w_ref.shape
    per = blocks // 3
    pt = -(-p_len // TILE)
    pu = -(-pt // n)
    lead = pt * TILE
    seq = tu * n * TILE
    rows = lead + seq
    counts = [min(n, pt - v * n) for v in range(pu)]
    peers = [partner(me, k) for k in range(n)]
    table = origin_table(m)
    last = m - 2

    def pick(place, values):
        total = jnp.int32(0)
        for e in range(n):
            total = jnp.maximum(total, jnp.where(slot_ref[e] == place, values(e), 0))
        return total

    def by_place(values):
        total = jnp.int32(0)
        for z in range(m):
            total = total + jnp.where(t == z, values[z], 0)
        return total

    origins = [by_place([table[z][i] for z in range(m)]) for i in range(m - 1)]

    def when(needed, act):
        if needed is None:
            act()
        else:
            pl.when(needed)(act)

    def describe(src, dst, send, recv, device):
        return pltpu.make_async_remote_copy(
            src_ref=src,
            dst_ref=dst,
            send_sem=send,
            recv_sem=recv,
            device_id=device,
            device_id_type=MESH,
        )

    def remote(src, dst, send, recv, device, needed=None):
        copy = describe(src, dst, send, recv, device)
        when(needed, copy.start)
        return copy

    sent = []

    def drain():
        while sent:
            copy, needed = sent.pop(0)
            when(needed, copy.wait_send)

    barrier = pltpu.get_barrier_semaphore()
    for z in range(m):
        for k in range(n):
            far = lax.rem(t + z, m)
            if z or k:
                pl.semaphore_signal(
                    barrier, inc=1, device_id=(peers[k], far), device_id_type=MESH
                )

    inputs = []
    for i, (src, dst) in enumerate((
        (text_hbm, text_ref), (prompts_hbm, prompts_ref), (cot_hbm, cot_ref),
        (gain_hbm, gain_ref), (cos_hbm, cos_ref), (sin_hbm, sin_ref),
    )):
        load = pltpu.make_async_copy(src, dst, semi.at[i])
        load.start()
        inputs.append(load)
    loads = []
    for i, hbm in enumerate((wq_hbm, wk_hbm, wv_hbm)):
        for g in range(per):
            at = i * per + g
            load = pltpu.make_async_copy(
                hbm.at[:, g * group : (g + 1) * group], w_ref.at[at], semw.at[at]
            )
            load.start()
            loads.append(load)

    inputs[0].wait()
    for u in range(tu):
        if u == 0:
            tz[t, me] = text_ref[0, me]
        else:
            trecv[u - 1, me] = text_ref[u, me]
    inputs[1].wait()
    whole = p_len // TILE
    spare = pu * n - pt
    for v in range(pu):
        full_tiles = max(0, min(n, whole - v * n))
        if full_tiles:
            pbuf[v, :full_tiles] = prompts_ref[
                v * n * TILE : (v * n + full_tiles) * TILE
            ].reshape(full_tiles, TILE, width)
    if p_len % TILE:
        rest = prompts_ref[whole * TILE : p_len].astype(f32)
        fill = jnp.zeros((TILE - p_len % TILE, width), f32)
        pbuf[whole // n, whole % n] = jnp.concatenate([rest, fill], axis=0).astype(bf16)
    if spare:
        pbuf[pu - 1, n - spare :] = jnp.zeros((spare, TILE, width), bf16)
    pl.semaphore_wait(barrier, n * m - 1)

    for k in range(1, n):
        remote(
            text_ref.at[0, peers[k]], tz.at[t, me], sem_t.at[0, 0], sem_t.at[1, 0],
            (peers[k], t),
        )
    for k in range(1, n):
        remote(
            text_ref.at[1:, peers[k]], trecv.at[:, me], sem_t.at[0, 1], sem_t.at[1, 1],
            (peers[k], t),
        )
    for k in range(1, n):
        remote(
            pbuf.at[:, peers[k]], precv.at[:, me], sem_p.at[0], sem_p.at[1], (peers[k], t)
        )
    spread_0 = describe(
        text_ref.at[0, 1:], tz.at[t, 1:n], sem_t.at[0, 0], sem_t.at[1, 0], (peers[1], t)
    )
    spread_t = describe(
        text_ref.at[1:, 1:], trecv.at[:, 1:], sem_t.at[0, 1], sem_t.at[1, 1], (peers[1], t)
    )
    spread_p = describe(
        pbuf.at[:, 1:], precv.at[:, 1:], sem_p.at[0], sem_p.at[1], (peers[1], t)
    )
    sent += [(spread_0, None), (spread_t, None), (spread_p, None)]
    for v in range(pu):
        precv[v, me] = pbuf[v, me]
    inputs[2].wait()
    cot_pad[:lead] = cot_ref[:lead]
    cot_pad[lead:] = cot_ref[p_len:].astype(f32).astype(bf16)
    sources = [pick(peers[k], lambda e: e) for k in range(n)]
    tasks_of = [pick(peers[k], lambda e: task_ref[e]) for k in range(n)]

    packed = slots < tu * n
    rank, ahead = [[jnp.int32(e) for e in range(n)]], jnp.int32(n)
    for u in range(1, tu):
        rank.append([])
        for e in range(n):
            live_tile = length_ref[e] > u * n * TILE
            rank[u].append(jnp.where(live_tile, ahead, -1) if packed else jnp.int32(u * n + e))
            ahead = ahead + jnp.where(live_tile, 1, 0)
    places = [
        [pick(peers[k], lambda e: jnp.maximum(rank[u][e], 0)) for k in range(n)]
        for u in range(tu)
    ]
    pieces = [(lo, min(lo + n, slots)) for lo in range(0, slots, n)]
    ready = {}
    for u in range(tu):
        ready.setdefault(min(u, len(pieces) - 1), []).append(u)

    ways = [(t < m - 1, lax.rem(t + 1, m)), (t > 0, lax.rem(t + m - 1, m))]

    def text_unit(z, g):
        lo, hi = pieces[g]
        return tz.at[z, lo:hi]

    def prompt_unit(z, v):
        return fullp.at[z, v, : counts[v]]

    units = [(text_unit, g) for g in range(len(pieces))] + [(prompt_unit, v) for v in range(pu)]
    own_sent = []

    def pass_own(i):
        ref = units[i][0](t, units[i][1])
        for w, (needed, far) in enumerate(ways):
            copy = remote(ref, ref, semz_own.at[w, i], semz_in.at[t, i], (me, far), needed)
            own_sent.append((copy, needed))

    spread_0.wait_recv()
    pass_own(0)
    spread_t.wait_recv()
    for g in range(1, len(pieces)):
        for i in range(*pieces[g]):
            if packed:
                spot = jnp.int32(0)
                for u in range(1, tu):
                    for e in range(n):
                        spot = jnp.where(rank[u][e] == i, (u - 1) * n + e, spot)
                tz[t, i] = trecv[spot // n, lax.rem(spot, n)]
            else:
                tz[t, i] = trecv[i // n - 1, i % n]
        pass_own(g)

    spread_p.wait_recv()
    for k in range(1, n):
        for v in range(pu):
            psend[k, v] = precv[v, tasks_of[k]]
        remote(psend.at[k], fullp.at[t, :, me], sem_c.at[0], sem_c.at[1], (peers[k], t))
    for v in range(pu):
        fullp[t, v, me] = precv[v, tasks_of[0]]
    collect_p = describe(
        psend.at[1:], fullp.at[t, :, 1:], sem_c.at[0], sem_c.at[1], (peers[1], t)
    )
    sent.append((collect_p, None))
    collected = {}

    def collect(i, z, lo, hi):
        for k in range(1, n):
            for u in range(lo, hi):
                tsend[i, k, u] = stage[places[u][k]]
            remote(
                tsend.at[i, k, lo:hi], fullt.at[z, lo:hi, me],
                sem_s.at[0, i, lo], sem_s.at[1, i, lo], (peers[k], t),
            )
        for u in range(lo, hi):
            fullt[z, u, me] = stage[places[u][0]]
        copy = describe(
            tsend.at[i, 1:, lo:hi], fullt.at[z, lo:hi, 1:],
            sem_s.at[0, i, lo], sem_s.at[1, i, lo], (peers[1], t),
        )
        collected[i, lo] = copy
        sent.append((copy, None))

    def finish(i):
        for key, copy in collected.items():
            if key[0] == i:
                copy.wait_recv()

    stage[...] = tz[t]
    collect(m - 1, t, 0, tu)
    collect_p.wait_recv()
    for v in range(pu):
        pass_own(len(pieces) + v)

    def take(z, lo, hi):
        parts = []
        if lo < lead:
            parts.append(fullp[z].reshape(pu * n * TILE, width)[lo : min(hi, lead)])
        if hi > lead:
            parts.append(fullt[z].reshape(seq, width)[max(lo, lead) - lead : hi - lead])
        return parts[0] if len(parts) == 1 else jnp.concatenate(parts, axis=0)

    def project(z, fresh, lo=0, hi=rows):
        wide = take(z, lo, hi).astype(f32)
        normed = (wide * inv_ref[lo:hi, :1] * gain_ref[z]).astype(bf16)
        deep = pl.ds(pl.multiple_of(z * width, width), width)

        def body(c, carry):
            for h in range(inner):
                b = c * inner + h
                product = dot_nn(normed, w_ref[b, deep, :])
                qkv[b, lo:hi] = product if fresh else qkv[b, lo:hi] + product
            return carry

        inner = blocks if lo or hi < rows else 3
        if inner == blocks:
            body(0, 0)
        else:
            lax.fori_loop(0, blocks // inner, body, 0)

    due = []

    def pump(i, lo, hi, step):
        z = origins[i]
        left = z < t
        needed = (left & (t < m - 1)) | (jnp.logical_not(left) & (t > 0))
        far = jnp.where(needed, jnp.where(left, t + 1, t - 1), z)
        for j in range(lo, hi):
            ref = units[j][0](z, units[j][1])
            copy = describe(ref, ref, semz_fwd.at[i, j], semz_in.at[z, j], (me, far))
            copy.wait_recv()
            when(needed, copy.start)
            sent.append((copy, needed))
            if j < len(pieces):
                lo_s, hi_s = pieces[j]
                stage[lo_s:hi_s] = tz[z, lo_s:hi_s]
                due.extend(ready.get(j, []))
                if due and (len(due) >= step or j == len(pieces) - 1):
                    collect(i, z, due[0], due[-1] + 1)
                    due.clear()

    half = len(pieces) // 2
    final = len(units)
    if m > 2:
        pump(0, 0, final, 2)
    finish(m - 1)
    own = take(t, 0, rows).astype(f32)
    square = jnp.broadcast_to(jnp.sum(own * own, axis=1, keepdims=True), (rows, 128))
    padded = squares.shape[2]
    square = jnp.concatenate([square, jnp.zeros((padded - rows, 128), f32)], axis=0)
    squares[0] = square.T[:8]
    shared = []
    for k in range(1, m):
        shared.append(
            remote(
                squares.at[0], squares.at[k], semq.at[0, k], semq.at[1, k],
                (me, lax.rem(t + k, m)),
            )
        )
    for i in range(1, last):
        pump(i, 0, final, 2)
    for load in inputs[3:] + loads:
        load.wait()
    for copy in shared:
        copy.wait_recv()
        sent.append((copy, None))
    square = squares[0]
    for k in range(1, m):
        square = square + squares[k]
    square = jnp.broadcast_to(square[:1], (128, padded)).T[:rows]
    inv_ref[...] = lax.rsqrt(square * (1.0 / model_width) + 1e-05)
    project(t, True)
    if m > 2:
        finish(0)
        project(origins[0], False)
    pump(last, 0, half, 1)
    for i in range(1, last):
        finish(i)
        project(origins[i], False)
    pump(last, half, len(pieces), 1)
    sent += own_sent
    drain()
    finish(last)
    project(origins[last], False, lead, rows)
    pump(last, len(pieces), final, 1)
    project(origins[last], False, 0, lead)

    limit = p_len + pick(me, lambda e: length_ref[e])
    scale = 1.0 / math.sqrt(HD)

    def positions(shape, axis):
        at = lax.broadcasted_iota(jnp.int32, shape, axis)
        return jnp.where(at < lead, jnp.where(at < p_len, at, PAD_POS), at - (lead - p_len))

    def heads(g, dots):
        cosine, sine = cos_ref[...], sin_ref[...]
        cosine_p, sine_p = cosine[:lead], sine[:lead]
        row_pos = positions((rows, 1), 0)
        col_pos = positions((1, rows), 1)
        allowed = (col_pos <= row_pos) & (col_pos < limit)
        live = row_pos < limit
        edge = min(rows, -(-lead // 128) * 128)
        for h in range(group // HD):
            at = slice(h * HD, (h + 1) * HD)
            far = pl.ds(pl.multiple_of(g * group + h * HD, HD), HD)
            q_raw, k_raw, v_raw = qkv[g, :, at], qkv[per + g, :, at], qkv[2 * per + g, :, at]
            v = v_raw.astype(bf16)
            q = (q_raw * cosine + pltpu.roll(q_raw, HD // 2, 1) * sine).astype(bf16)
            k = (k_raw * cosine + pltpu.roll(k_raw, HD // 2, 1) * sine).astype(bf16)
            scores = jnp.where(allowed, dot_nt(q, k) * scale, -1e30)
            peak = jnp.max(scores, axis=1, keepdims=True)
            weights = jnp.exp(scores - peak)
            probs = weights * (1.0 / jnp.sum(weights, axis=1, keepdims=True))
            low = probs.astype(bf16)
            mixed = jnp.where(live, dot_nn(low, v), 0.0)
            mixed = jnp.concatenate([mixed[:p_len], mixed[lead:]], axis=0)
            out_ref[:, far] = mixed.astype(bf16)
            upstream = jnp.where(live, cot_pad[:, far].astype(f32), 0.0).astype(bf16)
            grad_prob = dot_nt(upstream, v)
            delta = jnp.sum(probs * grad_prob, axis=1, keepdims=True)
            grad_score = (probs * (grad_prob - delta)).astype(bf16)
            gq = dot_nn(grad_score[:lead, :edge], k[:edge]) * scale
            gk = dot_tn(grad_score[:, :edge], q)[:lead] * scale
            gv = dot_tn(low[:, :edge], upstream)[:lead]
            gq = (gq * cosine_p - pltpu.roll(gq, HD // 2, 1) * sine_p).astype(bf16)
            gk = (gk * cosine_p - pltpu.roll(gk, HD // 2, 1) * sine_p).astype(bf16)
            gv = gv.astype(bf16)
            grads[g, :, at] = gq
            grads[per + g, :, at] = gk
            grads[2 * per + g, :, at] = gv
            along = gq.astype(f32) * q_raw[:lead] + gk.astype(f32) * k_raw[:lead]
            along = along + gv.astype(f32) * v_raw[:lead]
            dots = dots + jnp.sum(along, axis=1, keepdims=True)
        return dots

    dots = lax.fori_loop(0, per, heads, jnp.zeros((lead, 1), f32))
    inv = inv_ref[:lead, :1]
    factor = inv * inv * (dots * (1.0 / model_width))

    def holds(v, at):
        return None if counts[v] == n else v * n + at < pt

    for i in range(m):
        z = origins[last - i] if i <= last else t
        deep = pl.ds(pl.multiple_of(z * width, width), width)
        total = dot_nt(grads[0], w_ref[0, deep, :])
        for b in range(1, blocks):
            total = total + dot_nt(grads[b], w_ref[b, deep, :])
        prompt = fullp[z].reshape(pu * n * TILE, width)[:lead].astype(f32)
        value = inv * (total * gain_ref[z]) - prompt * factor
        value = value.astype(bf16).reshape(pt, TILE, width)
        for v in range(pu):
            part[i, v, : counts[v]] = value[v * n : v * n + counts[v]]
        for v in range(pu):
            for k in range(counts[v]):
                j = peers[k] if counts[v] == n else k
                away = None if i <= last else j != me
                if i > last and counts[v] == n and k == 0:
                    continue
                copy = remote(
                    part.at[i, v, j], pin.at[v, me, t], semg.at[i, v, k], semg_in.at[v], (j, z), away
                )
                sent.append((copy, away))
    homes = []
    for v in range(pu):
        home = pltpu.make_async_copy(part.at[m - 1, v, me], pin.at[v, me, t], semg_in.at[v])
        when(holds(v, me), home.start)

    tasks = [pick(s, lambda e: task_ref[e]) for s in range(n)]
    fourth = {}
    for v in range(pu):

        def gather(v=v):
            describe(
                pin.at[v], pin.at[v], semg.at[0, v, 0], semg_in.at[v], (peers[1], t)
            ).wait_recv()
            sums = [None] * n
            for s in range(n):
                total = pin[v, s, 0].astype(f32)
                for z in range(1, m):
                    total = total + pin[v, s, z].astype(f32)
                for k in range(n):
                    hit = jnp.where(tasks[s] == peers[k], total, 0.0)
                    sums[k] = hit if s == 0 else sums[k] + hit
            for k in range(n):
                if k == 0:
                    gout[v, me] = sums[k].astype(bf16)
                else:
                    send4[v, k] = sums[k].astype(bf16)

        when(holds(v, me), gather)
        for k in range(1, n):
            fourth[v, k] = remote(
                send4.at[v, k], gout.at[v, me], sem4.at[0, v, k], sem4.at[1, v, k],
                (peers[k], t), holds(v, me),
            )
            sent.append((fourth[v, k], holds(v, me)))
    for v in range(pu):
        for k in range(1, n):
            when(holds(v, peers[k]), fourth[v, k].wait_recv)
    for v in range(pu):
        for j in range(counts[v]):
            at = (v * n + j) * TILE
            size = min(TILE, p_len - at)
            grad_ref[at : at + size] = gout[v, j].astype(f32)[:size].reshape(size, 1, width)
    drain()


def fast_device(slots, number, text, prompts, gain, w_query, w_key, w_value, cotangent, task_of, lengths, slot):
    n, m = lax.axis_size("dp"), lax.axis_size("tensor")
    f32, bf16 = jnp.float32, jnp.bfloat16
    seq, width = text.shape[1], text.shape[2]
    p_len = prompts.shape[1]
    heads = w_query.shape[1]
    tu = seq // (TILE * n)
    pt = -(-p_len // TILE)
    pu = -(-pt // n)
    lead = pt * TILE
    rows = lead + seq
    row = np.arange(rows)
    pos = np.where(row < lead, np.where(row < p_len, row, 0), row - (lead - p_len))
    half = HD // 2
    angle = pos[:, None] * 10000.0 ** (-np.arange(half) / half)[None, :]
    cosine = np.concatenate([np.cos(angle)] * 2, axis=1).astype(np.float32)
    sine = np.concatenate([-np.sin(angle), np.sin(angle)], axis=1).astype(np.float32)
    group = 2 * HD if heads % (2 * HD) == 0 else HD
    blocks = 3 * (heads // group)
    units = -(-slots // n) + pu
    smem = pl.BlockSpec(memory_space=pltpu.SMEM)
    vmem = pl.BlockSpec(memory_space=pltpu.VMEM)
    hbm = pl.BlockSpec(memory_space=pl.ANY)
    dma = pltpu.SemaphoreType.DMA
    out, collected = pl.pallas_call(
        functools.partial(step_kernel, p_len, slots),
        out_shape=(
            jax.ShapeDtypeStruct((p_len + seq, heads), bf16),
            jax.ShapeDtypeStruct((p_len, 1, width), f32),
        ),
        in_specs=[smem] * 3 + [hbm] * 9,
        out_specs=(vmem, vmem),
        scratch_shapes=[
            pltpu.VMEM((blocks, m * width, group), bf16),
            pltpu.VMEM((tu, n, TILE, width), bf16),
            pltpu.VMEM((p_len, width), bf16),
            pltpu.VMEM((m, 1, width), f32),
            pltpu.VMEM((rows, HD), f32),
            pltpu.VMEM((rows, HD), f32),
            pltpu.VMEM((p_len + seq, heads), bf16),
            pltpu.VMEM((pu, n, TILE, width), bf16),
            pltpu.VMEM((pu, n, TILE, width), bf16),
            pltpu.VMEM((n, pu, TILE, width), bf16),
            pltpu.VMEM((m, pu, n, TILE, width), bf16),
            pltpu.VMEM((tu - 1, n, TILE, width), bf16),
            pltpu.VMEM((m, slots, TILE, width), bf16),
            pltpu.VMEM((slots, TILE, width), bf16),
            pltpu.VMEM((m, n, tu, TILE, width), bf16),
            pltpu.VMEM((m, tu, n, TILE, width), bf16),
            pltpu.VMEM((m, 8, -(-rows // 128) * 128), f32),
            pltpu.VMEM((blocks, rows, group), f32),
            pltpu.VMEM((blocks, lead, group), bf16),
            pltpu.VMEM((rows, 128), f32),
            pltpu.VMEM((rows, heads), bf16),
            pltpu.VMEM((m, pu, n, TILE, width), bf16),
            pltpu.VMEM((pu, n, m, TILE, width), bf16),
            pltpu.VMEM((pu, n, TILE, width), bf16),
            pltpu.VMEM((pu, n, TILE, width), bf16),
            dma((blocks,)),
            dma((6,)),
            dma((2, 2)),
            dma((2,)),
            dma((2,)),
            dma((2, m, tu)),
            dma((2, units)),
            dma((m, units)),
            dma((m, units)),
            dma((2, m)),
            dma((m, pu, n)),
            dma((pu,)),
            dma((2, pu, n)),
        ],
        compiler_params=pltpu.CompilerParams(
            collective_id=number, has_side_effects=True, vmem_limit_bytes=63 * 2**20
        ),
    )(
        slot, task_of, lengths, text.reshape(tu, n, TILE, width), prompts[0],
        gain.reshape(m, 1, width), jnp.asarray(cosine), jnp.asarray(sine), cotangent[0],
        w_query, w_key, w_value,
    )
    return (out[None], collected.reshape(1, p_len, width))


def fast_path(text, prompts, gain, w_query, w_key, w_value, cotangent, task_of, lengths, slot):
    n = lax.axis_size("dp")
    granule = TILE * n
    tiles = text.shape[1] // granule
    every = n * tiles
    few = every * 3 // 4
    args = (text, prompts, gain, w_query, w_key, w_value, cotangent, task_of, lengths, slot)
    live = jnp.sum((lengths + (granule - 1)) // granule)
    return lax.cond(
        live <= few,
        functools.partial(fast_device, few, 0),
        functools.partial(fast_device, every, 1),
        *args,
    )


def choose(text, prompts, *rest):
    n, m = lax.axis_size("dp"), lax.axis_size("tensor")
    seq, p_len = text.shape[1], prompts.shape[1]
    fits = (
        text.shape[0] == 1
        and prompts.shape[0] == 1
        and m >= 3
        and n >= 2
        and n & (n - 1) == 0
        and n <= 8
        and seq // (TILE * n) % 4 == 0
        and seq % (TILE * n) == 0
        and text.shape[2] % 128 == 0
    )
    return (fast_path if fits else on_device)(text, prompts, *rest)


def solution(mesh):
    in_specs = (
        P("dp", None, "tensor"),
        P("dp", None, "tensor"),
        P(),
        P(None, "tensor"),
        P(None, "tensor"),
        P(None, "tensor"),
        P("dp", None, "tensor"),
        P(),
        P(),
        P(),
    )
    out_specs = (P("dp", None, "tensor"), P("dp", None, "tensor"))
    return jax.shard_map(
        choose, mesh=mesh, in_specs=in_specs, out_specs=out_specs, check_vma=False
    )
```

```python
import functools
import math

import jax
import jax.numpy as jnp
import numpy as np
from jax import lax
from jax.experimental import pallas as pl
from jax.experimental.pallas import tpu as pltpu
from jax.sharding import PartitionSpec as P

HD = 128


def rope_tables(row_count):
    half_dim = HD // 2
    frequency = 10000.0 ** (-jnp.arange(half_dim, dtype=jnp.float32) / half_dim)
    angle_table = jnp.arange(row_count, dtype=jnp.float32)[:, None] * frequency[None, :]
    return (jnp.cos(angle_table), jnp.sin(angle_table))


def rotate(vectors, cosine_table, sine_table):
    half_dim = vectors.shape[-1] // 2
    first_half = vectors[..., :half_dim]
    second_half = vectors[..., half_dim:]
    cosine_b = cosine_table[:, None, :]
    sine_b = sine_table[:, None, :]
    return jnp.concatenate(
        [
            first_half * cosine_b - second_half * sine_b,
            second_half * cosine_b + first_half * sine_b,
        ],
        axis=-1,
    )


def unrotate(vectors, cosine_table, sine_table):
    half_dim = vectors.shape[-1] // 2
    first_half = vectors[..., :half_dim]
    second_half = vectors[..., half_dim:]
    cosine_b = cosine_table[:, None, :]
    sine_b = sine_table[:, None, :]
    return jnp.concatenate(
        [
            first_half * cosine_b + second_half * sine_b,
            second_half * cosine_b - first_half * sine_b,
        ],
        axis=-1,
    )


def transpose_product(grad_low, matrix):
    return lax.dot_general(
        grad_low, matrix, (((1,), (1,)), ((), ())), preferred_element_type=jnp.float32
    )


def attention_window(full_rows, gain, w_query, w_key, w_value, cotangent, valid_rows, prompt_len):
    batch_size, row_count, model_width = full_rows.shape
    head_count = w_query.shape[1] // HD
    wide_rows = full_rows.astype(jnp.float32)
    inv_rms = lax.rsqrt(jnp.mean(wide_rows * wide_rows, axis=-1) + 1e-05)
    normed = (
        (wide_rows * inv_rms[..., None] * gain)
        .astype(jnp.bfloat16)
        .reshape(batch_size * row_count, model_width)
    )
    cosine_table, sine_table = rope_tables(row_count)

    def project(matrix):
        return jnp.dot(normed, matrix, preferred_element_type=jnp.float32).reshape(
            batch_size, row_count, head_count, HD
        )

    queries = rotate(project(w_query), cosine_table, sine_table).astype(jnp.bfloat16)
    key_rows = rotate(project(w_key), cosine_table, sine_table).astype(jnp.bfloat16)
    value_rows = project(w_value).astype(jnp.bfloat16)
    score_scale = 1.0 / math.sqrt(HD)
    scores = (
        jnp.einsum("erhd,ekhd->ehrk", queries, key_rows, preferred_element_type=jnp.float32)
        * score_scale
    )
    rows_at = jnp.arange(row_count, dtype=jnp.int32)
    row_limit = prompt_len + valid_rows
    allowed = (rows_at[None, None, :] <= rows_at[None, :, None]) & (
        rows_at[None, None, :] < row_limit[:, None, None]
    )
    allowed = allowed[:, None]
    scores = jnp.where(allowed, scores, -1e30)
    row_peak = jnp.max(scores, axis=-1, keepdims=True)
    weights = jnp.where(allowed, jnp.exp(scores - row_peak), 0.0)
    probability = weights / jnp.sum(weights, axis=-1, keepdims=True)
    probs_low = probability.astype(jnp.bfloat16)
    live_rows = rows_at[None, :] < row_limit[:, None]
    mixed_rows = jnp.einsum(
        "ehrk,ekhd->erhd", probs_low, value_rows, preferred_element_type=jnp.float32
    )
    mixed_rows = jnp.where(live_rows[:, :, None, None], mixed_rows, 0.0)
    output = mixed_rows.reshape(batch_size, row_count, head_count * HD).astype(jnp.bfloat16)
    upstream = jnp.where(
        live_rows[:, :, None, None], cotangent.reshape(batch_size, row_count, head_count, HD), 0.0
    )
    grad_prob = jnp.einsum(
        "erhd,ekhd->ehrk", upstream, value_rows, preferred_element_type=jnp.float32
    )
    row_delta = jnp.sum(probability * grad_prob, axis=-1, keepdims=True)
    grad_score = (probability * (grad_prob - row_delta)).astype(jnp.bfloat16)
    grad_query = (
        jnp.einsum(
            "ehrk,ekhd->erhd",
            grad_score[:, :, :prompt_len, :],
            key_rows,
            preferred_element_type=jnp.float32,
        )
        * score_scale
    )
    grad_key = (
        jnp.einsum(
            "ehrk,erhd->ekhd",
            grad_score[:, :, :, :prompt_len],
            queries,
            preferred_element_type=jnp.float32,
        )
        * score_scale
    )
    grad_value = jnp.einsum(
        "ehrk,erhd->ekhd",
        probs_low[:, :, :, :prompt_len],
        upstream,
        preferred_element_type=jnp.float32,
    )
    cosine_lead = cosine_table[:prompt_len]
    sine_lead = sine_table[:prompt_len]
    flat_rows = batch_size * prompt_len
    grad_query = (
        unrotate(grad_query, cosine_lead, sine_lead)
        .astype(jnp.bfloat16)
        .reshape(flat_rows, head_count * HD)
    )
    grad_key = (
        unrotate(grad_key, cosine_lead, sine_lead)
        .astype(jnp.bfloat16)
        .reshape(flat_rows, head_count * HD)
    )
    grad_value = grad_value.astype(jnp.bfloat16).reshape(flat_rows, head_count * HD)
    grad_normed = (
        transpose_product(grad_query, w_query)
        + transpose_product(grad_key, w_key)
        + transpose_product(grad_value, w_value)
    )
    grad_normed = grad_normed.reshape(batch_size, prompt_len, model_width) * gain
    prompt_rows = wide_rows[:, :prompt_len]
    prompt_inv = inv_rms[:, :prompt_len, None]
    grad_rows = prompt_inv * grad_normed - prompt_rows * prompt_inv**3 * jnp.mean(
        grad_normed * prompt_rows, axis=-1, keepdims=True
    )
    return (output, grad_rows)


def on_device(text, prompts, gain, w_query, w_key, w_value, cotangent, task_of, lengths, slot):
    dp_count = lax.axis_size("dp")
    my_index = lax.axis_index("dp")
    ex_dev = text.shape[0]
    task_dev = prompts.shape[0]
    prompt_len = prompts.shape[1]
    example_count = slot.shape[0]
    task_count = task_dev * dp_count
    places = jnp.arange(example_count, dtype=jnp.int32)
    matching = slot[None, :] == places[:, None]
    task_slot = jnp.sum(jnp.where(matching, task_of[None, :], 0), axis=1)
    length_slot = jnp.sum(jnp.where(matching, lengths[None, :], 0), axis=1)
    first_place = my_index * ex_dev
    my_lengths = lax.dynamic_slice_in_dim(length_slot, first_place, ex_dev)
    task_ids = jnp.arange(task_count, dtype=jnp.int32)
    spread_text, spread_prompts = (
        lax.all_to_all(text, "dp", split_axis=2, concat_axis=0, tiled=True),
        lax.all_to_all(prompts, "dp", split_axis=2, concat_axis=0, tiled=True),
    )
    taking = matching.astype(jnp.bfloat16)
    placed_text = jnp.einsum(
        "se,erc->src", taking, spread_text, preferred_element_type=jnp.bfloat16
    )
    choosing = (task_slot[:, None] == task_ids[None, :]).astype(jnp.bfloat16)
    placed_prompts = jnp.einsum(
        "st,tpc->spc", choosing, spread_prompts, preferred_element_type=jnp.bfloat16
    )
    placed = jnp.concatenate([placed_prompts, placed_text], axis=1)
    placed = placed.reshape(dp_count, ex_dev, placed.shape[1], placed.shape[2])
    local_rows = lax.all_to_all(placed, "dp", split_axis=0, concat_axis=3, tiled=True)[0]
    full_rows = lax.all_gather(local_rows, "tensor", axis=2, tiled=True)
    output, grad_part = attention_window(
        full_rows, gain, w_query, w_key, w_value, cotangent, my_lengths, prompt_len
    )
    grad_share = lax.psum_scatter(grad_part, "tensor", scatter_dimension=2, tiled=True)
    spread_grads = lax.all_to_all(grad_share, "dp", split_axis=2, concat_axis=0, tiled=True)
    collecting = (task_ids[:, None] == task_slot[None, :]).astype(jnp.float32)
    per_task = jnp.einsum("ts,spc->tpc", collecting, spread_grads, precision=lax.Precision.HIGHEST)
    prompt_grad = lax.all_to_all(per_task, "dp", split_axis=0, concat_axis=2, tiled=True)
    return (output, prompt_grad)


MESH = pl.DeviceIdType.MESH
PAD_POS = 1 << 20
TILE = 8


def dot_nn(a, b):
    return jnp.dot(a, b, preferred_element_type=jnp.float32)


def dot_nt(a, b):
    return lax.dot_general(a, b, (((1,), (1,)), ((), ())), preferred_element_type=jnp.float32)


def dot_tn(a, b):
    return lax.dot_general(a, b, (((0,), (0,)), ((), ())), preferred_element_type=jnp.float32)


def partner(me, k):
    bit, peer = 1, me
    while bit <= k:
        if k & bit:
            peer = peer + bit - 2 * bit * lax.rem(me // bit, 2)
        bit *= 2
    return peer


def origin_table(m):
    table = []
    for t in range(m):
        others = [z for z in range(m) if z != t]
        others.sort(key=lambda z: (abs(z - t), (z < t) == (2 * t < m)))
        table.append(others)
    return table


def step_kernel(
    p_len, slots, slot_ref, task_ref, length_ref, text_hbm, prompts_hbm, gain_hbm, cos_hbm, sin_hbm,
    cot_hbm, wq_hbm, wk_hbm, wv_hbm, out_hbm, grad_hbm,
    w_ref, text_ref, prompts_ref, gain_ref, cos_ref, sin_ref, cot_ref,
    pbuf, precv, psend, fullp, trecv, tz, stage, tsend, fullt, squares, qkv, grads, inv_ref, cot_pad,
    part, pin, send4, gout, vsend, acc, out_ref, grad_ref,
    semw, semi, semo, sem_t, sem_p, sem_c, sem_s, sem_v, semz_own, semz_fwd, semz_in, semq, semg, semg_in, sem4,
):
    n, m = lax.axis_size("dp"), lax.axis_size("tensor")
    me, t = lax.axis_index("dp"), lax.axis_index("tensor")
    f32, bf16 = jnp.float32, jnp.bfloat16
    tu, _, _, width = text_ref.shape
    blocks, model_width, group = w_ref.shape
    per = blocks // 3
    pt = -(-p_len // TILE)
    pu = -(-pt // n)
    lead = pt * TILE
    seq = tu * n * TILE
    rows = lead + seq
    counts = [min(n, pt - v * n) for v in range(pu)]
    zf = sum(c == n for c in counts)
    base = n * (1 + zf)
    peers = [partner(me, k) for k in range(n)]
    table = origin_table(m)
    last = m - 2

    def pick(place, values):
        total = jnp.int32(0)
        for e in range(n):
            total = jnp.maximum(total, jnp.where(slot_ref[e] == place, values(e), 0))
        return total

    def by_place(values):
        total = jnp.int32(0)
        for z in range(m):
            total = total + jnp.where(t == z, values[z], 0)
        return total

    origins = [by_place([table[z][i] for z in range(m)]) for i in range(m - 1)]

    def when(needed, act):
        if needed is None:
            act()
        else:
            pl.when(needed)(act)

    def describe(src, dst, send, recv, device):
        return pltpu.make_async_remote_copy(
            src_ref=src,
            dst_ref=dst,
            send_sem=send,
            recv_sem=recv,
            device_id=device,
            device_id_type=MESH,
        )

    def remote(src, dst, send, recv, device, needed=None):
        copy = describe(src, dst, send, recv, device)
        when(needed, copy.start)
        return copy

    sent = []

    def drain():
        while sent:
            copy, needed = sent.pop(0)
            when(needed, copy.wait_send)

    barrier = pltpu.get_barrier_semaphore()
    for z in range(m):
        for k in range(n):
            far = lax.rem(t + z, m)
            if z or k:
                pl.semaphore_signal(
                    barrier, inc=1, device_id=(peers[k], far), device_id_type=MESH
                )

    inputs = []
    for i, (src, dst) in enumerate((
        (text_hbm, text_ref), (prompts_hbm, prompts_ref), (cot_hbm, cot_ref),
        (gain_hbm, gain_ref), (cos_hbm, cos_ref), (sin_hbm, sin_ref),
    )):
        load = pltpu.make_async_copy(src, dst, semi.at[i])
        load.start()
        inputs.append(load)
    loads = []
    for i, hbm in enumerate((wq_hbm, wk_hbm, wv_hbm)):
        for g in range(per):
            at = i * per + g
            load = pltpu.make_async_copy(
                hbm.at[:, g * group : (g + 1) * group], w_ref.at[at], semw.at[at]
            )
            load.start()
            loads.append(load)

    inputs[0].wait()
    for u in range(tu):
        if u == 0:
            tz[t, me] = text_ref[0, me]
        else:
            trecv[u - 1, me] = text_ref[u, me]
    inputs[1].wait()
    whole = p_len // TILE
    spare = pu * n - pt
    for v in range(pu):
        full_tiles = max(0, min(n, whole - v * n))
        if full_tiles:
            pbuf[v, :full_tiles] = prompts_ref[
                v * n * TILE : (v * n + full_tiles) * TILE
            ].reshape(full_tiles, TILE, width)
    if p_len % TILE:
        rest = prompts_ref[whole * TILE : p_len].astype(f32)
        fill = jnp.zeros((TILE - p_len % TILE, width), f32)
        pbuf[whole // n, whole % n] = jnp.concatenate([rest, fill], axis=0).astype(bf16)
    if spare:
        pbuf[pu - 1, n - spare :] = jnp.zeros((spare, TILE, width), bf16)
    pl.semaphore_wait(barrier, n * m - 1)

    for k in range(1, n):
        remote(
            text_ref.at[0, peers[k]], tz.at[t, me], sem_t.at[0, 0], sem_t.at[1, 0],
            (peers[k], t),
        )
    for v in range(zf):
        for k in range(1, n):
            remote(
                pbuf.at[v, peers[k]], tz.at[t, n + v * n + me], sem_p.at[0, v], sem_p.at[1, v],
                (peers[k], t),
            )
    for k in range(1, n):
        remote(
            text_ref.at[1:, peers[k]], trecv.at[:, me], sem_t.at[0, 1], sem_t.at[1, 1],
            (peers[k], t),
        )
    if zf < pu:
        for k in range(1, n):
            remote(
                pbuf.at[zf:, peers[k]], precv.at[:, me], sem_p.at[0, zf], sem_p.at[1, zf],
                (peers[k], t),
            )
    spread_0 = describe(
        text_ref.at[0, 1:], tz.at[t, 1:n], sem_t.at[0, 0], sem_t.at[1, 0], (peers[1], t)
    )
    spread_v = [
        describe(
            pbuf.at[v, 1:], tz.at[t, n + v * n + 1 : 2 * n + v * n], sem_p.at[0, v],
            sem_p.at[1, v], (peers[1], t),
        )
        for v in range(zf)
    ]
    spread_t = describe(
        text_ref.at[1:, 1:], trecv.at[:, 1:], sem_t.at[0, 1], sem_t.at[1, 1], (peers[1], t)
    )
    settled = [(copy, None) for copy in [spread_0, spread_t] + spread_v]
    if zf < pu:
        spread_p = describe(
            pbuf.at[zf:, 1:], precv.at[:, 1:], sem_p.at[0, zf], sem_p.at[1, zf], (peers[1], t)
        )
        settled.append((spread_p, None))
    for v in range(pu):
        if v < zf:
            tz[t, n + v * n + me] = pbuf[v, me]
        else:
            precv[v - zf, me] = pbuf[v, me]
    inputs[2].wait()
    cot_pad[:lead] = cot_ref[:lead]
    cot_pad[lead:] = cot_ref[p_len:].astype(f32).astype(bf16)
    sources = [pick(peers[k], lambda e: e) for k in range(n)]
    tasks_of = [pick(peers[k], lambda e: task_ref[e]) for k in range(n)]

    packed = slots < tu * n
    rank, ahead = [[jnp.int32(e) for e in range(n)]], jnp.int32(base)
    for u in range(1, tu):
        rank.append([])
        for e in range(n):
            live_tile = length_ref[e] > u * n * TILE
            rank[u].append(jnp.where(live_tile, ahead, -1) if packed else jnp.int32(base + (u - 1) * n + e))
            ahead = ahead + jnp.where(live_tile, 1, 0)
    places = [
        [pick(peers[k], lambda e: jnp.maximum(rank[u][e], 0)) for k in range(n)]
        for u in range(tu)
    ]
    end = base + slots - n
    pieces = [(lo, min(lo + n, end)) for lo in range(base, end, n)]
    ready = {0: [0]}
    for u in range(1, tu):
        ready.setdefault(zf + min(u, len(pieces)), []).append(u)

    ways = [(t < m - 1, lax.rem(t + 1, m)), (t > 0, lax.rem(t + m - 1, m))]

    ranges = [(lo, lo + n) for lo in range(0, base, n)] + pieces
    first_piece, first_part = 1 + zf, len(ranges)

    def text_unit(z, g):
        lo, hi = ranges[g]
        return tz.at[z, lo:hi]

    def prompt_unit(z, v):
        return fullp.at[z, v, : counts[v]]

    units = [(text_unit, g) for g in range(len(ranges))]
    units += [(prompt_unit, v) for v in range(zf, pu)]
    final = len(units)
    own_sent = []

    def pass_own(i):
        ref = units[i][0](t, units[i][1])
        for w, (needed, far) in enumerate(ways):
            copy = remote(ref, ref, semz_own.at[w, i], semz_in.at[t, i], (me, far), needed)
            own_sent.append((copy, needed))

    spread_0.wait_recv()
    pass_own(0)
    for v in range(zf):
        spread_v[v].wait_recv()
        pass_own(1 + v)
    spread_t.wait_recv()
    for g in range(first_piece, first_part):
        for i in range(*ranges[g]):
            if packed:
                spot = jnp.int32(0)
                for u in range(1, tu):
                    for e in range(n):
                        spot = jnp.where(rank[u][e] == i, (u - 1) * n + e, spot)
                tz[t, i] = trecv[spot // n, lax.rem(spot, n)]
            else:
                tz[t, i] = trecv[(i - base) // n, (i - base) % n]
        pass_own(g)

    if zf < pu:
        spread_p.wait_recv()
        for k in range(1, n):
            for v in range(zf, pu):
                psend[k, v - zf] = precv[v - zf, tasks_of[k]]
            remote(
                psend.at[k], fullp.at[t, zf:, me], sem_c.at[0], sem_c.at[1], (peers[k], t)
            )
        for v in range(zf, pu):
            fullp[t, v, me] = precv[v - zf, tasks_of[0]]
        collect_p = describe(
            psend.at[1:], fullp.at[t, zf:, 1:], sem_c.at[0], sem_c.at[1], (peers[1], t)
        )
        settled.append((collect_p, None))
    collected = {}

    def collect(i, z, lo, hi):
        for k in range(1, n):
            for u in range(lo, hi):
                tsend[i, k, u] = stage[places[u][k]]
            remote(
                tsend.at[i, k, lo:hi], fullt.at[z, lo:hi, me],
                sem_s.at[0, i, lo], sem_s.at[1, i, lo], (peers[k], t),
            )
        for u in range(lo, hi):
            fullt[z, u, me] = stage[places[u][0]]
        copy = describe(
            tsend.at[i, 1:, lo:hi], fullt.at[z, lo:hi, 1:],
            sem_s.at[0, i, lo], sem_s.at[1, i, lo], (peers[1], t),
        )
        collected[i, lo] = copy
        (settled if i < last or i > last else sent).append((copy, None))

    def collect_v(i, z, v):
        for k in range(1, n):
            vsend[i, v, k] = stage[n + v * n + tasks_of[k]]
            remote(
                vsend.at[i, v, k], fullp.at[z, v, me], sem_v.at[0, i, v], sem_v.at[1, i, v],
                (peers[k], t),
            )
        fullp[z, v, me] = stage[n + v * n + tasks_of[0]]
        copy = describe(
            vsend.at[i, v, 1:], fullp.at[z, v, 1:], sem_v.at[0, i, v], sem_v.at[1, i, v],
            (peers[1], t),
        )
        collected[i, -1 - v] = copy
        (settled if i < last or i > last else sent).append((copy, None))

    def finish(i, late=None):
        for key, copy in collected.items():
            if key[0] == i and (late is None or (key[1] > 0) == late):
                copy.wait_recv()

    stage[...] = tz[t]
    for v in range(zf):
        collect_v(m - 1, t, v)
    collect(m - 1, t, 0, tu)
    if zf < pu:
        collect_p.wait_recv()
    for i in range(first_part, final):
        pass_own(i)

    def take(z, lo, hi):
        parts = []
        if lo < lead:
            parts.append(fullp[z].reshape(pu * n * TILE, width)[lo : min(hi, lead)])
        if hi > lead:
            first, count = (max(lo, lead) - lead) // (n * TILE), (hi - lead) // (n * TILE)
            parts.append(fullt[z, first:count].reshape((count - first) * n * TILE, width))
        return parts[0] if len(parts) == 1 else jnp.concatenate(parts, axis=0)

    def project(z, fresh, lo=0, hi=rows):
        wide = take(z, lo, hi).astype(f32)
        normed = (wide * inv_ref[lo:hi, :1] * gain_ref[z]).astype(bf16)
        deep = pl.ds(pl.multiple_of(z * width, width), width)

        def body(c, carry):
            for h in range(inner):
                b = c * inner + h
                product = dot_nn(normed, w_ref[b, deep, :])
                qkv[b, lo:hi] = product if fresh else qkv[b, lo:hi] + product
            return carry

        inner = blocks if lo or hi < rows else 3
        if inner == blocks:
            body(0, 0)
        else:
            lax.fori_loop(0, blocks // inner, body, 0)

    due = []

    def onward(i):
        z = origins[i]
        left = z < t
        needed = (left & (t < m - 1)) | (jnp.logical_not(left) & (t > 0))
        return z, needed, jnp.where(needed, jnp.where(left, t + 1, t - 1), z)

    def forward(i, order):
        z, needed, far = onward(i)

        @pl.when(needed)
        def _():
            for j in order:
                ref = units[j][0](z, units[j][1])
                copy = describe(ref, ref, semz_fwd.at[i, j], semz_in.at[z, j], (me, far))
                copy.wait_recv()
                copy.start()

        for j in order:
            ref = units[j][0](z, units[j][1])
            copy = describe(ref, ref, semz_fwd.at[i, j], semz_in.at[z, j], (me, far))
            sent.append((copy, needed))

    def pump(i, order, step):
        z, needed, far = onward(i)
        for j in order:
            ref = units[j][0](z, units[j][1])
            copy = describe(ref, ref, semz_fwd.at[i, j], semz_in.at[z, j], (me, far))
            if i == 0:
                copy.wait_recv()
                when(needed, copy.start)
                sent.append((copy, needed))
            else:
                pl.when(jnp.logical_not(needed))(copy.wait_recv)
            if j < first_part:
                lo_s, hi_s = ranges[j]
                stage[lo_s:hi_s] = tz[z, lo_s:hi_s]
                if 0 < j < first_piece:
                    collect_v(i, z, j - 1)
                due.extend(ready.get(j, []))
                if due and (len(due) >= step or j == first_part - 1):
                    collect(i, z, due[0], due[-1] + 1)
                    due.clear()

    every = list(range(final))
    texts = every[first_piece:first_part]
    half = max(1, len(texts) // 2)
    if m > 2:
        pump(0, every, 2)
    finish(m - 1)
    own = take(t, 0, rows).astype(f32)
    square = jnp.broadcast_to(jnp.sum(own * own, axis=1, keepdims=True), (rows, 128))
    padded = squares.shape[2]
    square = jnp.concatenate([square, jnp.zeros((padded - rows, 128), f32)], axis=0)
    squares[0] = square.T[:8]
    shared = []
    for k in range(1, m):
        shared.append(
            remote(
                squares.at[0], squares.at[k], semq.at[0, k], semq.at[1, k],
                (me, lax.rem(t + k, m)),
            )
        )
    for i in range(1, last):
        forward(i, every)
    for i in range(1, last):
        pump(i, every, 2)
    for load in inputs[3:] + loads:
        load.wait()
    for copy in shared:
        copy.wait_recv()
        sent.append((copy, None))
    square = squares[0]
    for k in range(1, m):
        square = square + squares[k]
    square = jnp.broadcast_to(square[:1], (128, padded)).T[:rows]
    inv_ref[...] = lax.rsqrt(square * (1.0 / model_width) + 1e-05)
    project(t, True)
    if m > 2:
        finish(0)
        project(origins[0], False)
    forward(last, texts)
    pump(last, texts[:half], 1)
    for i in range(1, last):
        finish(i)
        project(origins[i], False)
    forward(last, every[:first_piece] + every[first_part:])
    pump(last, texts[half:], 1)
    pump(last, every[:first_piece], 1)
    finish(last, True)
    project(origins[last], False, lead + n * TILE, rows)
    pump(last, every[first_part:], 1)
    finish(last, False)
    project(origins[last], False, 0, lead + n * TILE)

    limit = p_len + pick(me, lambda e: length_ref[e])
    scale = 1.0 / math.sqrt(HD)

    def positions(shape, axis):
        at = lax.broadcasted_iota(jnp.int32, shape, axis)
        return jnp.where(at < lead, jnp.where(at < p_len, at, PAD_POS), at - (lead - p_len))

    def heads(g, dots):
        cosine, sine = cos_ref[...], sin_ref[...]
        cosine_p, sine_p = cosine[:lead], sine[:lead]
        row_pos = positions((rows, 1), 0)
        col_pos = positions((1, rows), 1)
        live = row_pos < limit
        edge = min(rows, -(-lead // 128) * 128)
        cuts = [0] + [] + [rows]
        spans = [
            (lo, hi, min(rows, -(-hi // 128) * 128)) for lo, hi in zip(cuts[:-1], cuts[1:])
        ]
        masks = {
            lo: (col_pos[:, :keys] <= row_pos[lo:hi]) & (col_pos[:, :keys] < limit)
            for lo, hi, keys in spans
        }
        for h in range(group // HD):
            at = slice(h * HD, (h + 1) * HD)
            far = pl.ds(pl.multiple_of(g * group + h * HD, HD), HD)
            q_raw, k_raw, v_raw = qkv[g, :, at], qkv[per + g, :, at], qkv[2 * per + g, :, at]
            v = v_raw.astype(bf16)
            q = (q_raw * cosine + pltpu.roll(q_raw, HD // 2, 1) * sine).astype(bf16)
            k = (k_raw * cosine + pltpu.roll(k_raw, HD // 2, 1) * sine).astype(bf16)
            upstream = jnp.where(live, cot_pad[:, far].astype(f32), 0.0).astype(bf16)
            mixed, gk, gv = [], 0.0, 0.0
            for lo, hi, keys in spans:
                allowed = masks[lo]
                scores = jnp.where(allowed, dot_nt(q[lo:hi], k[:keys]) * scale, -1e30)
                peak = jnp.max(scores, axis=1, keepdims=True)
                weights = jnp.exp(scores - peak)
                probs = weights * (1.0 / jnp.sum(weights, axis=1, keepdims=True))
                low = probs.astype(bf16)
                mixed.append(dot_nn(low, v[:keys]))
                grad_prob = dot_nt(upstream[lo:hi], v[:keys])
                delta = jnp.sum(probs * grad_prob, axis=1, keepdims=True)
                grad_score = (probs * (grad_prob - delta)).astype(bf16)
                if lo == 0:
                    gq = dot_nn(grad_score[:lead, :edge], k[:edge]) * scale
                gk = gk + dot_tn(grad_score[:, :edge], q[lo:hi])[:lead]
                gv = gv + dot_tn(low[:, :edge], upstream[lo:hi])[:lead]
            gk = gk * scale
            mixed = jnp.where(live, jnp.concatenate(mixed, axis=0), 0.0)
            mixed = jnp.concatenate([mixed[:p_len], mixed[lead:]], axis=0)
            out_ref[:, far] = mixed.astype(bf16)
            gq = (gq * cosine_p - pltpu.roll(gq, HD // 2, 1) * sine_p).astype(bf16)
            gk = (gk * cosine_p - pltpu.roll(gk, HD // 2, 1) * sine_p).astype(bf16)
            gv = gv.astype(bf16)
            grads[g, :, at] = gq
            grads[per + g, :, at] = gk
            grads[2 * per + g, :, at] = gv
            along = gq.astype(f32) * q_raw[:lead] + gk.astype(f32) * k_raw[:lead]
            along = along + gv.astype(f32) * v_raw[:lead]
            dots = dots + jnp.sum(along, axis=1, keepdims=True)
        return dots

    dots = lax.fori_loop(0, per, heads, jnp.zeros((lead, 1), f32))
    store_out = pltpu.make_async_copy(out_ref, out_hbm, semo.at[0])
    store_out.start()
    inv = inv_ref[:lead, :1]
    factor = inv * inv * (dots * (1.0 / model_width))

    def holds(v, at):
        return None if counts[v] == n else v * n + at < pt

    def partial(i, v, n_k, act):
        z = sum(jnp.where(i == at, origins[last - at], 0) for at in range(m - 1))
        z = jnp.where(i <= last, z, t)
        j = peers[n_k] if counts[v] == n else n_k
        copy = describe(
            part.at[i, v, j], pin.at[v, me, t], semg.at[i, v, n_k], semg_in.at[v], (j, z)
        )
        pl.when((i <= last) | (j != me))(lambda: act(copy))

    def back(i, carry):
        z = sum(jnp.where(i == at, origins[last - at], 0) for at in range(m - 1))
        z = jnp.where(i <= last, z, t)
        deep = pl.ds(pl.multiple_of(z * width, width), width)
        total = dot_nt(grads[0], w_ref[0, deep, :])
        for b in range(1, blocks):
            total = total + dot_nt(grads[b], w_ref[b, deep, :])
        acc[...] = total
        prompt = fullp[z].reshape(pu * n * TILE, width)[:lead].astype(f32)
        value = inv * (acc[...] * gain_ref[z]) - prompt * factor
        value = value.astype(bf16).reshape(pt, TILE, width)
        for v in range(pu):
            part[i, v, : counts[v]] = value[v * n : v * n + counts[v]]
        for v in range(pu):
            for k in range(counts[v]):
                partial(i, v, k, lambda copy: copy.start())
        return carry

    lax.fori_loop(0, m, back, 0)
    sent += settled + own_sent
    drain()
    homes = []
    for v in range(pu):
        home = pltpu.make_async_copy(part.at[m - 1, v, me], pin.at[v, me, t], semg_in.at[v])
        when(holds(v, me), home.start)

    tasks = [pick(s, lambda e: task_ref[e]) for s in range(n)]
    fourth = {}
    for v in range(pu):

        def gather(v=v):
            describe(
                pin.at[v], pin.at[v], semg.at[0, v, 0], semg_in.at[v], (peers[1], t)
            ).wait_recv()
            sums = [None] * n
            for s in range(n):
                total = pin[v, s, 0].astype(f32)
                for z in range(1, m):
                    total = total + pin[v, s, z].astype(f32)
                for k in range(n):
                    hit = jnp.where(tasks[s] == peers[k], total, 0.0)
                    sums[k] = hit if s == 0 else sums[k] + hit
            for k in range(n):
                if k == 0:
                    gout[v, me] = sums[k].astype(bf16)
                else:
                    send4[v, k] = sums[k].astype(bf16)

        when(holds(v, me), gather)
        for k in range(1, n):
            fourth[v, k] = remote(
                send4.at[v, k], gout.at[v, me], sem4.at[0, v, k], sem4.at[1, v, k],
                (peers[k], t), holds(v, me),
            )
            sent.append((fourth[v, k], holds(v, me)))
    for v in range(pu):
        for k in range(1, n):
            when(holds(v, peers[k]), fourth[v, k].wait_recv)
    for v in range(pu):
        for j in range(counts[v]):
            at = (v * n + j) * TILE
            size = min(TILE, p_len - at)
            grad_ref[at : at + size] = gout[v, j].astype(f32)[:size]
    store_grad = pltpu.make_async_copy(grad_ref, grad_hbm, semo.at[1])
    store_grad.start()
    drain()

    def settle(i, carry):
        for v in range(pu):
            for k in range(counts[v]):
                partial(i, v, k, lambda copy: copy.wait_send())
        return carry

    lax.fori_loop(0, m, settle, 0)
    store_out.wait()
    store_grad.wait()


def fast_device(slots, number, text, prompts, gain, w_query, w_key, w_value, cotangent, task_of, lengths, slot):
    n, m = lax.axis_size("dp"), lax.axis_size("tensor")
    f32, bf16 = jnp.float32, jnp.bfloat16
    seq, width = text.shape[1], text.shape[2]
    p_len = prompts.shape[1]
    heads = w_query.shape[1]
    tu = seq // (TILE * n)
    pt = -(-p_len // TILE)
    pu = -(-pt // n)
    lead = pt * TILE
    rows = lead + seq
    row = np.arange(rows)
    pos = np.where(row < lead, np.where(row < p_len, row, 0), row - (lead - p_len))
    half = HD // 2
    angle = pos[:, None] * 10000.0 ** (-np.arange(half) / half)[None, :]
    cosine = np.concatenate([np.cos(angle)] * 2, axis=1).astype(np.float32)
    sine = np.concatenate([-np.sin(angle), np.sin(angle)], axis=1).astype(np.float32)
    group = 2 * HD if heads % (2 * HD) == 0 else HD
    blocks = 3 * (heads // group)
    zf = pt // n
    units = -(-slots // n) + pu
    smem = pl.BlockSpec(memory_space=pltpu.SMEM)
    vmem = pl.BlockSpec(memory_space=pltpu.VMEM)
    hbm = pl.BlockSpec(memory_space=pl.ANY)
    dma = pltpu.SemaphoreType.DMA
    out, collected = pl.pallas_call(
        functools.partial(step_kernel, p_len, slots),
        out_shape=(
            jax.ShapeDtypeStruct((p_len + seq, heads), bf16),
            jax.ShapeDtypeStruct((p_len, width), f32),
        ),
        in_specs=[smem] * 3 + [hbm] * 9,
        out_specs=(hbm, hbm),
        scratch_shapes=[
            pltpu.VMEM((blocks, m * width, group), bf16),
            pltpu.VMEM((tu, n, TILE, width), bf16),
            pltpu.VMEM((p_len, width), bf16),
            pltpu.VMEM((m, 1, width), f32),
            pltpu.VMEM((rows, HD), f32),
            pltpu.VMEM((rows, HD), f32),
            pltpu.VMEM((p_len + seq, heads), bf16),
            pltpu.VMEM((pu, n, TILE, width), bf16),
            pltpu.VMEM((max(1, pu - zf), n, TILE, width), bf16),
            pltpu.VMEM((n, max(1, pu - zf), TILE, width), bf16),
            pltpu.VMEM((m, pu, n, TILE, width), bf16),
            pltpu.VMEM((tu - 1, n, TILE, width), bf16),
            pltpu.VMEM((m, slots + zf * n, TILE, width), bf16),
            pltpu.VMEM((slots + zf * n, TILE, width), bf16),
            pltpu.VMEM((m, n, tu, TILE, width), bf16),
            pltpu.VMEM((m, tu, n, TILE, width), bf16),
            pltpu.VMEM((m, 8, -(-rows // 128) * 128), f32),
            pltpu.VMEM((blocks, rows, group), f32),
            pltpu.VMEM((blocks, lead, group), bf16),
            pltpu.VMEM((rows, 128), f32),
            pltpu.VMEM((rows, heads), bf16),
            pltpu.VMEM((m, pu, n, TILE, width), bf16),
            pltpu.VMEM((pu, n, m, TILE, width), bf16),
            pltpu.VMEM((pu, n, TILE, width), bf16),
            pltpu.VMEM((pu, n, TILE, width), bf16),
            pltpu.VMEM((m, max(1, zf), n, TILE, width), bf16),
            pltpu.VMEM((lead, width), f32),
            pltpu.VMEM((p_len + seq, heads), bf16),
            pltpu.VMEM((p_len, width), f32),
            dma((blocks,)),
            dma((6,)),
            dma((2,)),
            dma((2, 2)),
            dma((2, pu + 1)),
            dma((2,)),
            dma((2, m, tu)),
            dma((2, m, max(1, zf))),
            dma((2, units)),
            dma((m, units)),
            dma((m, units)),
            dma((2, m)),
            dma((m, pu, n)),
            dma((pu,)),
            dma((2, pu, n)),
        ],
        compiler_params=pltpu.CompilerParams(
            collective_id=number, has_side_effects=True, vmem_limit_bytes=63 * 2**20
        ),
    )(
        slot, task_of, lengths, text.reshape(tu, n, TILE, width), prompts[0],
        gain.reshape(m, 1, width), jnp.asarray(cosine), jnp.asarray(sine), cotangent[0],
        w_query, w_key, w_value,
    )
    return (out[None], collected.reshape(1, p_len, width))


def fast_path(text, prompts, gain, w_query, w_key, w_value, cotangent, task_of, lengths, slot):
    n = lax.axis_size("dp")
    granule = TILE * n
    tiles = text.shape[1] // granule
    every = n * tiles
    few = every * 3 // 4
    args = (text, prompts, gain, w_query, w_key, w_value, cotangent, task_of, lengths, slot)
    live = jnp.sum((lengths + (granule - 1)) // granule)
    return lax.cond(
        live <= few,
        functools.partial(fast_device, few, 0),
        functools.partial(fast_device, every, 1),
        *args,
    )


def choose(text, prompts, *rest):
    n, m = lax.axis_size("dp"), lax.axis_size("tensor")
    seq, p_len = text.shape[1], prompts.shape[1]
    fits = (
        text.shape[0] == 1
        and prompts.shape[0] == 1
        and m >= 3
        and n >= 2
        and n & (n - 1) == 0
        and n <= 8
        and seq // (TILE * n) % 4 == 0
        and seq % (TILE * n) == 0
        and text.shape[2] % 128 == 0
    )
    return (fast_path if fits else on_device)(text, prompts, *rest)


def solution(mesh):
    in_specs = (
        P("dp", None, "tensor"),
        P("dp", None, "tensor"),
        P(),
        P(None, "tensor"),
        P(None, "tensor"),
        P(None, "tensor"),
        P("dp", None, "tensor"),
        P(),
        P(),
        P(),
    )
    out_specs = (P("dp", None, "tensor"), P("dp", None, "tensor"))
    return jax.shard_map(
        choose, mesh=mesh, in_specs=in_specs, out_specs=out_specs, check_vma=False
    )
```
